128 devices in a mesh: flow: 64 (over x, y, z), group: 2 (over core).
Axes of the slice: x: 4, y: 4, z: 4, core: 2. Of those that a mesh axis runs over, the one named last changes fastest.
Arguments:
- density: float32 [256, 32, 256], P('flow', 'group'), may hold values from 0.8 to 1.2
- velocity: float32 [3, 256, 32, 256], P(None, 'flow', 'group'), may hold values from -0.5 to 0.5
- pressure: float32 [256, 32, 256], P('flow', 'group'), may hold values from 0.7 to 1.3
- wave_state: float32 [4, 8, 8, 8, 16384], P(None, None, None, None, ('flow', 'group')), may hold values from -1.8 to 1.8
- tables: float32 [4, 512, 512], replicated, may hold values from -0.75 to 0.75
- margin_element: int32 [128, 256], P(('flow', 'group')), may hold values from 0 to 16383, as said below
- margin_block: int32 [128, 256], P(('flow', 'group')), may hold values from 0 to 31
- margin_table: int32 [128, 256], P(('flow', 'group')), may hold values from 0 to 3
Outputs:
- flow_state: float32 [5, 256, 32, 256], P(None, 'flow', 'group')
- wave_out: float32 [4, 8, 8, 8, 16384], P(None, None, None, None, ('flow', 'group'))
- forcing: float32 [3, 8, 8, 8, 16384], P(None, None, None, None, ('flow', 'group'))
The draws below stay inside these ranges and needn't reach their ends.
Inputs may be any that keep to these rules, and one draw needn't show every extreme that they name: `margin_element`: global element ids; element e belongs to the device at position e // 128 along flow then group. In every device's row at most 4 entries name elements of one owner, and some owner receives exactly 4 entries from it.
All inputs are finite; a program needn't handle non-finite values.
Results may differ from the reference program's by a relative error of at most 0.0003.
Values sent between devices are 32-bit elements; how exact they have to be, the bound alone decides.
No kernel may reach another device: no remote copies, remote signals or barrier semaphores. Data moves between devices by JAX's collectives and lax.ppermute only.
A program may use at most 128 MiB of HBM per device.

```python
import jax
import jax.numpy as jnp
import numpy as np
from jax import lax

NP = 8
CX = 4
CY = 16
NZ = 256
EY = 8
EZ = 16
CAP = 4
NW = 4
STEPS = 2
OV_DEV = 256
NX = 256
NY = 32
NBLK = 32
ELEMENTS = 16384
N_FLOW = 64
N_GROUP = 2


def draw_margin_element(key, part):
    devices = N_FLOW * N_GROUP
    slot_total = devices * CAP
    center_key, choose_key = jax.random.split(jax.random.fold_in(key, 11))
    center = jax.random.randint(center_key, (), 0, devices)
    hot_width = max(devices // 16, 2)

    def one_sender(sender_key, sender):
        sub_keys = jax.random.split(sender_key, 3)
        owner_index = jnp.arange(slot_total, dtype=jnp.int32) // CAP
        offset = (owner_index - center) % devices
        priority = jax.random.randint(sub_keys[0], (slot_total,), 0, 2)
        priority = jnp.where(offset < hot_width, 2, priority)
        priority = jnp.where(owner_index == (center + 3 * sender + hot_width) % devices, 3, priority)
        tiebreak = jax.random.permutation(sub_keys[1], slot_total)
        scores = priority * (slot_total + 1) + tiebreak
        chosen = jnp.sort(jax.lax.top_k(scores, OV_DEV)[1])
        element = chosen // CAP * (EY * EZ) + jax.random.randint(sub_keys[2], (OV_DEV,), 0, EY * EZ)
        return element.astype(jnp.int32)
    sender_keys = jax.random.split(choose_key, devices)
    return jax.vmap(one_sender)(sender_keys, jnp.arange(devices, dtype=jnp.int32))


def plant(drawn, stream_key, low, top_value):
    spot = [jax.random.randint(jax.random.fold_in(stream_key, axis), (), 0, length) for axis, length in enumerate(drawn.shape)]
    longest = drawn.shape.index(max(drawn.shape))
    beside = spot[:longest] + [(spot[longest] + 1) % drawn.shape[longest]] + spot[longest + 1:]
    return drawn.at[tuple(spot)].set(low).at[tuple(beside)].set(top_value)


def levels(key, shape, cuts, low, high):
    def one(position, shards_of):
        steps = jax.random.uniform(jax.random.fold_in(jax.random.fold_in(key, 6), position), (shards_of,), jnp.float32, low / len(cuts), high / len(cuts))
        return jnp.repeat(jnp.exp(steps), shape[position] // shards_of).reshape((-1,) + (1,) * (len(shape) - position - 1))

    factor_of = one(*cuts[0])
    for cut in cuts[1:]:
        factor_of = factor_of * one(*cut)
    return factor_of


def centred(rng, shape, spread, reach, cuts=(), kind=jnp.bfloat16):
    values = jax.random.normal(rng, shape, jnp.float32) * spread
    if len(cuts) > 0:
        values = levels(rng, shape, cuts, -0.22, 0.18) * values
    return jnp.clip(values, min=-reach, max=reach).astype(kind)


def setup_inputs(seed: int = 0) -> dict:
    streams_of = jax.random.split(jax.random.key(seed), 9)
    density = jnp.clip(0.8 + 0.40000004 * jax.random.uniform(streams_of[0], (NX, NY, NZ), jnp.float32) ** levels(streams_of[0], (NX, NY, NZ), ((0, 64), (1, 2)), -0.2, 0.2), 0.8, 1.2)
    velocity = jnp.clip(jax.random.uniform(streams_of[1], (3, NX, NY, NZ), jnp.float32, -0.5, 0.5) * levels(streams_of[1], (3, NX, NY, NZ), ((1, 64), (2, 2)), -0.4, 0.0), -0.5, 0.5)
    pressure = jnp.clip(0.7 + 0.59999996 * jax.random.uniform(streams_of[2], (NX, NY, NZ), jnp.float32) ** levels(streams_of[2], (NX, NY, NZ), ((0, 64), (1, 2)), -0.2, 0.2), 0.7, 1.3)
    wave_state = centred(streams_of[3], (4, NP, NP, NP, ELEMENTS), 0.3, 1.8, ((4, 128),), jnp.float32)
    tables = centred(streams_of[4], (NW, NP**3, NP**3), 0.125, 0.75, (), jnp.float32)
    margin_element = draw_margin_element(jax.random.fold_in(streams_of[8], 71), 0)
    margin_block = plant(jax.random.randint(streams_of[6], (N_FLOW * N_GROUP, OV_DEV), 0, NBLK), jax.random.fold_in(streams_of[6], 1), 0, NBLK - 1).astype(jnp.int32)
    margin_table = plant(jax.random.randint(streams_of[7], (N_FLOW * N_GROUP, OV_DEV), 0, NW), jax.random.fold_in(streams_of[7], 1), 0, NW - 1).astype(jnp.int32)
    return {"density": density, "velocity": velocity, "pressure": pressure, "wave_state": wave_state, "tables": tables, "margin_element": margin_element, "margin_block": margin_block, "margin_table": margin_table}


GAMMA = 1.4
DT_FLOW = 0.08
ACOUSTIC_STEP = 0.01
MAXIMUM_DEGREE = lax.Precision.HIGHEST

def legendre_pair(quadrature_nodes, degree):
    previous = np.ones(quadrature_nodes.shape[0])
    current = quadrature_nodes * 1.0
    for order in range(2, degree + 1):
        previous, current = (current, ((2 * order - 1) * quadrature_nodes * current - (order - 1) * previous) / order)
    return (previous, current)

def lobatto(point_count):
    degree = point_count - 1
    quadrature_nodes = -np.cos(np.pi * np.arange(point_count) / degree)
    for sweep in range(60):
        previous, current = legendre_pair(quadrature_nodes, degree)
        quadrature_nodes = quadrature_nodes - (quadrature_nodes * current - previous) / (point_count * current)
    previous, values = legendre_pair(quadrature_nodes, degree)
    quadrature_weights = 2.0 / (degree * (degree + 1) * values ** 2)
    identity = np.eye(point_count)
    differ = quadrature_nodes[:, None] - quadrature_nodes[None, :] + identity
    matrix = values[:, None] / values[None, :] / differ * (1.0 - identity)
    matrix[0, 0] = -degree * (degree + 1) / 4.0
    matrix[-1, -1] = degree * (degree + 1) / 4.0
    return (matrix, float(quadrature_weights[0]))

def physical(fields):
    density = fields[0]
    velocity = fields[1:4] / density
    pressure = (GAMMA - 1.0) * (fields[4] - 0.5 * density * lax.optimization_barrier(jnp.sum(velocity * velocity, axis=0)))
    return (density, velocity, pressure)

def euler_flux(fields, velocity, pressure, direction):
    normal = velocity[direction]
    components = [fields[0] * normal]
    for column in range(3):
        product = fields[1 + column] * normal
        if column == direction:
            product = product + pressure
        components.append(product)
    components.append((fields[4] + pressure) * normal)
    return jnp.stack(components)

def rusanov(left_side, right_side, direction):
    left_rho, left_vel, left_pre = physical(left_side)
    right_rho, right_vel, right_pre = physical(right_side)
    wave_speed = jnp.maximum(jnp.abs(left_vel[direction]) + jnp.sqrt(GAMMA * left_pre / left_rho), jnp.abs(right_vel[direction]) + jnp.sqrt(GAMMA * right_pre / right_rho))
    return 0.5 * (euler_flux(left_side, left_vel, left_pre, direction) + euler_flux(right_side, right_vel, right_pre, direction)) - 0.5 * wave_speed * (right_side - left_side)

def flow_rate(fields):
    tendency = jnp.zeros_like(fields)
    for direction in range(3):
        axis_index = direction + 1
        face_flux = rusanov(fields, jnp.roll(fields, -1, axis_index), direction)
        tendency = tendency - (face_flux - jnp.roll(face_flux, 1, axis_index))
    return tendency

def lamb_vector(fields):
    velocity = fields[1:4] / fields[0]
    slope_x = 0.5 * (jnp.roll(velocity, -1, 1) - jnp.roll(velocity, 1, 1))
    slope_y = 0.5 * (jnp.roll(velocity, -1, 2) - jnp.roll(velocity, 1, 2))
    slope_z = 0.5 * (jnp.roll(velocity, -1, 3) - jnp.roll(velocity, 1, 3))
    curl_x = slope_y[2] - slope_z[1]
    curl_y = slope_z[0] - slope_x[2]
    curl_z = slope_x[1] - slope_y[0]
    return jnp.stack([curl_y * velocity[2] - curl_z * velocity[1], curl_z * velocity[0] - curl_x * velocity[2], curl_x * velocity[1] - curl_y * velocity[0]])

def derivative(values, derive, direction):
    forms = ('ai,ijke->ajke', 'aj,ijke->iake', 'ak,ijke->ijae')
    return jnp.einsum(forms[direction], derive, values, precision=MAXIMUM_DEGREE)

def place_lifts(lower_lift, upper_lift, direction, point_count):
    middle_shape = list(upper_lift.shape)
    middle_shape.insert(direction, point_count - 2)
    middle = jnp.zeros(middle_shape, upper_lift.dtype)
    return jnp.concatenate([jnp.expand_dims(lower_lift, direction), middle, jnp.expand_dims(upper_lift, direction)], axis=direction)

def wave_rate(wave_field, forcing, upper_of, lower_of):
    point_count = wave_field.shape[1]
    matrix, end_weight = lobatto(point_count)
    derive = jnp.asarray(matrix, jnp.float32)
    pressure = wave_field[0]
    pressure_rate = jnp.zeros_like(pressure)
    velocity_tendency = []
    last = point_count - 1
    for direction in range(3):
        normal = wave_field[1 + direction]
        lower_face = jnp.stack([jnp.take(pressure, 0, axis=direction), jnp.take(normal, 0, axis=direction)])
        upper_face = jnp.stack([jnp.take(pressure, last, axis=direction), jnp.take(normal, last, axis=direction)])
        above_face = upper_of(lower_face, direction)
        below_face = lower_of(upper_face, direction)
        upper_pressure_flux = 0.5 * (upper_face[1] + above_face[1]) - 0.5 * (above_face[0] - upper_face[0])
        upper_normal_flux = 0.5 * (upper_face[0] + above_face[0]) - 0.5 * (above_face[1] - upper_face[1])
        lower_pressure_flux = 0.5 * (below_face[1] + lower_face[1]) - 0.5 * (lower_face[0] - below_face[0])
        lower_normal_flux = 0.5 * (below_face[0] + lower_face[0]) - 0.5 * (lower_face[1] - below_face[1])
        pressure_lift = place_lifts((lower_pressure_flux - lower_face[1]) / end_weight, -(upper_pressure_flux - upper_face[1]) / end_weight, direction, point_count)
        normal_lift = place_lifts((lower_normal_flux - lower_face[0]) / end_weight, -(upper_normal_flux - upper_face[0]) / end_weight, direction, point_count)
        pressure_rate = pressure_rate - derivative(normal, derive, direction) + pressure_lift
        velocity_tendency.append(-derivative(pressure, derive, direction) + normal_lift + forcing[direction])
    return jnp.stack([pressure_rate] + velocity_tendency)

def runge_kutta(start, rate, step_size):
    first_section = start + step_size * rate(start)
    second_section = 0.75 * start + 0.25 * (first_section + step_size * rate(first_section))
    return start / 3.0 + 2.0 / 3.0 * (second_section + step_size * rate(second_section))

def project(source, tables, margin_element, margin_block, margin_table):
    devices = N_FLOW * N_GROUP
    node_count = NP ** 3
    sorted_entries = source.reshape(3, N_FLOW, CX, N_GROUP, CY, NZ).transpose(0, 1, 3, 2, 4, 5)
    sorted_entries = sorted_entries.reshape(3, devices, NBLK, node_count)
    mapped_values = jnp.einsum('cdbn,tnm->tcdbm', sorted_entries, tables, precision=MAXIMUM_DEGREE)
    owners = jnp.broadcast_to(jnp.arange(devices, dtype=jnp.int32)[:, None], margin_block.shape)
    pieces = mapped_values[margin_table, :, owners, margin_block, :]
    summed = jax.ops.segment_sum(pieces.reshape(devices * OV_DEV, 3 * node_count), margin_element.reshape(-1), num_segments=ELEMENTS)
    return summed.reshape(ELEMENTS, 3, NP, NP, NP).transpose(1, 2, 3, 4, 0)

def shifted(faces, direction, offset):
    grid_view = faces.reshape(faces.shape[:3] + (N_FLOW * N_GROUP, EY, EZ))
    return jnp.roll(grid_view, offset, 3 + direction).reshape(faces.shape)

def reference(density, velocity, pressure, wave_state, tables, margin_element, margin_block, margin_table):
    momentum = density[None] * velocity
    energy = pressure / (GAMMA - 1.0) + 0.5 * density * lax.optimization_barrier(jnp.sum(velocity * velocity, axis=0))
    fields = jnp.concatenate([density[None], momentum, energy[None]], axis=0)
    wave_field = wave_state
    forcing = jnp.zeros((3, NP, NP, NP, ELEMENTS), jnp.float32)
    for step_index in range(STEPS):
        forcing = project(lamb_vector(fields), tables, margin_element, margin_block, margin_table)
        fields = runge_kutta(fields, flow_rate, DT_FLOW)
        wave_field = runge_kutta(wave_field, lambda current: wave_rate(current, forcing, lambda faces, direction: shifted(faces, direction, -1), lambda faces, direction: shifted(faces, direction, 1)), ACOUSTIC_STEP)
    return (fields, wave_field, forcing)
```

```python
import jax
import jax.numpy as jnp
import numpy as np
from jax import lax
from jax.experimental import pallas as pl
from jax.experimental.pallas import tpu as pltpu
from jax.sharding import PartitionSpec as P


NP = 8
EZ = 16
CAP = 4
GAMMA = 1.4
DT_FLOW = 0.08
DT_WAVE = 0.01
F32 = jnp.float32
BF16 = jnp.bfloat16
AXES = ("flow", "group")
VMEM_LIMIT = 26 * 2**20
WHOLE_VMEM = 58 * 2**20


def legendre_pair(nodes, degree):
    previous = np.ones(nodes.shape[0])
    current = nodes * 1.0
    for order in range(2, degree + 1):
        previous, current = (
            current,
            ((2 * order - 1) * nodes * current - (order - 1) * previous) / order,
        )
    return (previous, current)


def lobatto(point_count):
    degree = point_count - 1
    nodes = -np.cos(np.pi * np.arange(point_count) / degree)
    for _ in range(60):
        previous, current = legendre_pair(nodes, degree)
        nodes = nodes - (nodes * current - previous) / (point_count * current)
    previous, values = legendre_pair(nodes, degree)
    weights = 2.0 / (degree * (degree + 1) * values**2)
    identity = np.eye(point_count)
    differ = nodes[:, None] - nodes[None, :] + identity
    matrix = values[:, None] / values[None, :] / differ * (1.0 - identity)
    matrix[0, 0] = -degree * (degree + 1) / 4.0
    matrix[-1, -1] = degree * (degree + 1) / 4.0
    return (matrix.astype(np.float32), float(weights[0]))


MATRIX, END_WEIGHT = lobatto(NP)
LIFT = 0.5 / END_WEIGHT


def sds(*shape, dtype=F32):
    return jax.ShapeDtypeStruct(shape, dtype)


def call(body, out_shape, flops, scratch=(), specs=None, out_specs=None, limit=VMEM_LIMIT):
    kinds = {"s": pltpu.SMEM, "v": pltpu.VMEM, "h": pltpu.HBM}
    extra = {}
    if specs is not None:
        extra["in_specs"] = [pl.BlockSpec(memory_space=kinds[k]) for k in specs]
    if out_specs is not None:
        extra["out_specs"] = pl.BlockSpec(memory_space=kinds[out_specs])
    return pl.pallas_call(
        body,
        out_shape=out_shape,
        scratch_shapes=list(scratch),
        cost_estimate=pl.CostEstimate(flops=flops, bytes_accessed=4_000_000, transcendentals=0),
        compiler_params=pltpu.CompilerParams(vmem_limit_bytes=limit),
        **extra,
    )


def halves(value):
    high = value.astype(BF16)
    return high, (value - high.astype(F32)).astype(BF16)


def dot(left, right, dims=((1,), (0,))):
    return lax.dot_general(left, right, (dims, ((), ())), preferred_element_type=F32)


def fields_body(rho_ref, vel_ref, pre_ref, f_ref):
    rho = rho_ref[...]
    v = [vel_ref[d] for d in range(3)]
    kinetic = v[0] * v[0] + v[1] * v[1] + v[2] * v[2]
    f_ref[0] = rho
    for d in range(3):
        f_ref[1 + d] = rho * v[d]
    f_ref[4] = pre_ref[...] / (GAMMA - 1.0) + 0.5 * rho * kinetic


def slots_body(me_ref, mb_ref, mt_ref, sel_ref, lab_ref, *, blocks):
    entries = me_ref.shape[1]
    devices = lab_ref.shape[0]
    shape = (devices, entries)
    owner = me_ref[...] >> 7
    place = (me_ref[...] & 127).astype(F32)
    lane = lax.broadcasted_iota(jnp.int32, shape, 0)
    owned = (lane == owner).astype(F32)
    before = lax.broadcasted_iota(jnp.int32, (entries, entries), 0) < lax.broadcasted_iota(
        jnp.int32, (entries, entries), 1
    )
    ahead = dot(owned.astype(BF16), before.astype(F32).astype(BF16))
    rank = jnp.sum(owned * ahead, axis=0, keepdims=True)
    combo = (lane == mt_ref[...] * blocks + mb_ref[...]).astype(F32).astype(BF16)
    for s in range(CAP):
        mine = jnp.where(rank == float(s), owned, 0.0).astype(BF16)
        pick = dot(mine, combo, ((1,), (1,))).astype(BF16)
        half = devices // 2
        for h in range(2):
            at = (h * CAP + s) * half
            for side in range(2):
                sel_ref[at : at + half, side * 128 : (side + 1) * 128] = pick[
                    h * half : (h + 1) * half
                ]
    spread = jnp.where(lane.astype(F32) == rank, place + 1.0, 0.0).astype(BF16)
    lab_ref[...] = dot(owned.astype(BF16), spread, ((1,), (1,)))


def pack_body(
    flag,
    own_ref,
    part_ref,
    even_ref,
    odd_ref,
    tab_hbm,
    sel_ref,
    lab_ref,
    out_hbm,
    src,
    mp,
    tab,
    out,
    sems,
):
    planes, rows, width = own_ref.shape[1:]
    tables, nodes = tab.shape[0], tab.shape[1]
    blocks = 128 // tables
    loads = [pltpu.make_async_copy(tab_hbm.at[t], tab.at[t], sems.at[t]) for t in range(tables)]
    for load in loads:
        load.start()
    low_flow = flag[0] == 0

    def turn(value, by):
        return pltpu.roll(value, by % width, 1)

    for x in range(planes):
        v = [own_ref[d, x] for d in range(3)]

        def along_x(d):
            if x == 0:
                below = jnp.where(low_flow, odd_ref[d, 0], even_ref[d, 0])
            else:
                below = own_ref[d, x - 1]
            if x == planes - 1:
                above = jnp.where(low_flow, even_ref[d, 0], odd_ref[d, 0])
            else:
                above = own_ref[d, x + 1]
            return 0.5 * (above - below)

        def along_y(d):
            both = jnp.concatenate([v[d], part_ref[d, x]], axis=0)
            up = pltpu.roll(both, 2 * rows - 1, 0)[:rows]
            down = pltpu.roll(both, 1, 0)[:rows]
            return 0.5 * (up - down)

        def along_z(d):
            return 0.5 * (turn(v[d], -1) - turn(v[d], 1))

        curl = (
            along_y(2) - along_z(1),
            along_z(0) - along_x(2),
            along_x(1) - along_y(0),
        )
        for c in range(3):
            a, b = (c + 1) % 3, (c + 2) % 3
            base = (c * planes + x) * rows
            lamb = curl[a] * v[b] - curl[b] * v[a]
            src[0, base : base + rows, :] = lamb[:, :128]
            src[1, base : base + rows, :] = lamb[:, 128:]
    count = 3 * blocks
    split = [
        halves(src[half, pl.ds(start, count, stride=2), :])
        for start in range(2)
        for half in range(2)
    ]
    left = jnp.concatenate(
        [
            jnp.concatenate([h for h, _ in split], axis=1),
            jnp.concatenate([l for _, l in split], axis=1),
        ],
        axis=0,
    )
    for t in range(tables):
        loads[t].wait()
        high, low = halves(tab[t])
        wide = dot(left, high)
        mapped = wide[:count] + wide[count:] + dot(left[:count], low)
        for c in range(3):
            high, low = halves(mapped[c * blocks : (c + 1) * blocks])
            mp[c, t * blocks : (t + 1) * blocks, :] = high
            mp[c, 128 + t * blocks : 128 + (t + 1) * blocks, :] = low
    devices = lab_ref.shape[0]
    half = devices // 2
    groups = nodes // 128
    stride = 3 * groups * CAP + 1
    out[pl.ds(stride - 1, devices, stride=stride), :] = lab_ref[...]
    stores = []
    for h in range(2):
        for c in range(3):
            filled = dot(sel_ref[h * CAP * half : (h + 1) * CAP * half, :], mp[c])
            for s in range(CAP):
                for m in range(groups):
                    row = h * half * stride + CAP * (c * groups + m) + s
                    out[pl.ds(row, half, stride=stride), :] = filled[
                        s * half : (s + 1) * half, m * 128 : (m + 1) * 128
                    ]
        part = pl.ds(h * half * stride, half * stride)
        store = pltpu.make_async_copy(out.at[part], out_hbm.at[part], sems.at[tables + h])
        store.start()
        stores.append(store)
    for store in stores:
        store.wait()


def primitives(s):
    inverse = 1.0 / s[0]
    v = [s[1 + d] * inverse for d in range(3)]
    kinetic = v[0] * v[0] + v[1] * v[1] + v[2] * v[2]
    p = (GAMMA - 1.0) * (s[4] - 0.5 * s[0] * kinetic)
    return v, p, jnp.sqrt(GAMMA * p * inverse)


def flux_of(s, v, p, d, k):
    if k == 0:
        return s[1 + d]
    if k == 4:
        return (s[4] + p) * v
    product = s[k] * v
    return product + p if k == 1 + d else product


def flow_stage(src, base, dst, prim, first, last, weights, shift=0, rows=None):
    a_weight, b_weight = weights

    def prepare(x, carry):
        v, p, sound = primitives([src[k, x] for k in range(5)])
        for d in range(3):
            prim[d, x] = v[d]
        prim[3, x] = p
        prim[4, x] = sound
        return carry

    lax.fori_loop(first - 1, last + 1, prepare, 0)

    def advance(x, carry):
        s = [src[k, x] for k in range(5)]
        total = []
        sound = prim[4, x]
        p = prim[3, x]
        up = [src[k, x + 1] for k in range(5)]
        down = [src[k, x - 1] for k in range(5)]
        v, vu, vd = prim[0, x], prim[0, x + 1], prim[0, x - 1]
        speed = jnp.abs(v) + sound
        fast_u = jnp.maximum(speed, jnp.abs(vu) + prim[4, x + 1])
        fast_d = jnp.maximum(speed, jnp.abs(vd) + prim[4, x - 1])
        pu, pd = prim[3, x + 1], prim[3, x - 1]
        for k in range(5):
            jump = fast_u * (up[k] - s[k]) - fast_d * (s[k] - down[k])
            total.append(flux_of(up, vu, pu, 0, k) - flux_of(down, vd, pd, 0, k) - jump)
        for d, axis in ((1, 0), (2, 1)):
            size = s[0].shape[axis]
            v = prim[d, x]
            speed = jnp.abs(v) + sound
            fast = jnp.maximum(speed, pltpu.roll(speed, size - 1, axis))
            for k in range(5):
                flux = flux_of(s, v, p, d, k)
                face = flux + pltpu.roll(flux, size - 1, axis)
                face = face - fast * (pltpu.roll(s[k], size - 1, axis) - s[k])
                total[k] = total[k] + (face - pltpu.roll(face, 1, axis))
        for k in range(5):
            value = b_weight * s[k] - (0.5 * DT_FLOW * b_weight) * total[k]
            if a_weight is not None:
                value = value + a_weight * base[k, x]
            if rows is not None:
                value = value[:rows]
            dst[k, x - shift] = value
        return carry

    lax.fori_loop(first, last, advance, 0)


STAGES = ((None, 1.0), (0.75, 0.25), (1.0 / 3.0, 2.0 / 3.0))


def assemble(flag, mine, other, s0):
    own, _, _ = mine
    planes, rows = own.shape[1], own.shape[2]
    above = jnp.where(flag[0] == 0, 2 * planes, 0)
    starts = (planes, above, 2 * planes - above)
    for start, a, b in zip(starts, mine, other):
        for i in range(planes):
            for k in range(5):
                s0[k, start + i, :rows] = a[k, i]
                s0[k, start + i, rows:] = b[k, i]


def first_flow_body(flag, *refs):
    mine, other = refs[:3], refs[3:6]
    new_own, new_part, own_ref, part_ref, lo_ref, hi_ref = refs[6:12]
    s0, s1, s2, prim = refs[12:]
    planes, rows = mine[0].shape[1], mine[0].shape[2]
    assemble(flag, mine, other, s0)
    wide = 3 * planes
    flow_stage(s0, None, s1, prim, 1, wide - 1, STAGES[0])
    flow_stage(s1, s0, s2, prim, 2, wide - 2, STAGES[1])
    flow_stage(s2, s0, s1, prim, 3, wide - 3, STAGES[2])
    for i in range(-1, planes + 1):
        x = planes + i
        inverse = 1.0 / s1[0, x]
        v = [s1[1 + d, x] * inverse for d in range(3)]
        for d in range(3):
            if i == -1:
                lo_ref[d, 0] = v[d][:rows]
            elif i == planes:
                hi_ref[d, 0] = v[d][:rows]
            else:
                own_ref[d, i] = v[d][:rows]
                part_ref[d, i] = v[d][rows:]
        if 0 <= i < planes:
            for k in range(5):
                new_own[k, i] = s1[k, x, :rows]
                new_part[k, i] = s1[k, x, rows:]


def last_flow_body(flag, *refs):
    mine, other, out_ref = refs[:3], refs[3:6], refs[6]
    s0, s1, s2, prim = refs[7:]
    planes, rows = mine[0].shape[1], mine[0].shape[2]
    assemble(flag, mine, other, s0)
    wide = 3 * planes
    flow_stage(s0, None, s1, prim, 2, wide - 2, STAGES[0])
    flow_stage(s1, s0, s2, prim, 3, wide - 3, STAGES[1])
    flow_stage(s2, s0, out_ref, prim, planes, 2 * planes, STAGES[2], shift=planes, rows=rows)


def derive(values):
    half = NP // 2
    even = [values[i] + values[NP - 1 - i] for i in range(half)]
    odd = [values[i] - values[NP - 1 - i] for i in range(half)]
    tops, bottoms = [], []
    for a in range(half):
        plus = minus = None
        for i in range(half):
            ce = 0.5 * float(MATRIX[a, i] + MATRIX[a, NP - 1 - i])
            co = 0.5 * float(MATRIX[a, i] - MATRIX[a, NP - 1 - i])
            te, to = ce * even[i], co * odd[i]
            plus = te if plus is None else plus + te
            minus = to if minus is None else minus + to
        tops.append(plus + minus)
        bottoms.append(minus - plus)
    return tops + bottoms[::-1]


def along_middle(ps, us, lanes):
    p = derive(ps)
    below, above = (ps[-1], -ps[0]) if us is None else (ps[-1] + us[-1], us[0] - ps[0])
    own_low, own_high = (ps[0], -ps[-1]) if us is None else (ps[0] + us[0], us[-1] - ps[-1])
    low = LIFT * (pltpu.roll(below, EZ, 1) - own_low)
    high = LIFT * (pltpu.roll(above, lanes - EZ, 1) - own_high)
    dp = [None] * NP if us is None else [-u for u in derive(us)]
    du = [-value for value in p]
    dp[0] = low if dp[0] is None else dp[0] + low
    dp[-1] = -high if dp[-1] is None else dp[-1] - high
    du[0] = du[0] + low
    du[-1] = du[-1] + high
    return dp, du


def inner_maker(coef, lanes):
    lane = lax.broadcasted_iota(jnp.int32, (NP, lanes), 1)
    row = lax.broadcasted_iota(jnp.int32, (NP, lanes), 0)
    firsts = (lane & (EZ - 1)) == 0
    lasts = (lane & (EZ - 1)) == EZ - 1
    is_low = row == 0
    lift_u = jnp.where(is_low | (row == NP - 1), LIFT, 0.0)
    lift_p = jnp.where(is_low, LIFT, jnp.where(row == NP - 1, -LIFT, 0.0))

    def slope(value):
        total = coef[0] * value
        for k in range(1, NP):
            total = total + coef[k] * pltpu.roll(value, NP - k, 0)
        return total

    def jump_of(p, u):
        up, down = (p, -p) if u is None else (u + p, u - p)
        edge = jnp.where(is_low, pltpu.roll(up, 1, 0), pltpu.roll(down, NP - 1, 0))
        from_low = jnp.where(firsts, pltpu.roll(edge, lanes + 1 - EZ, 1), pltpu.roll(edge, 1, 1))
        from_high = jnp.where(
            lasts, pltpu.roll(edge, EZ - 1, 1), pltpu.roll(edge, lanes - 1, 1)
        )
        return jnp.where(is_low, from_low - up, from_high - down)

    def both(p, u, want_u=True):
        jump = jump_of(p, u)
        dp = lift_p * jump if u is None else lift_p * jump - slope(u)
        return dp, (lift_u * jump - slope(p)) if want_u else None

    return both


def local_rate(s, r, coef, forcing=None):
    lanes = s.shape[-1]

    def first(j, carry):
        p = derive([s[0, i, j] for i in range(NP)])
        u = derive([s[1, i, j] for i in range(NP)])
        for i in range(NP):
            r[0, i, j] = -u[i]
            r[1, i, j] = -p[i] if forcing is None else forcing[0, i, j] - p[i]
        return carry

    lax.fori_loop(0, NP, first, 0)
    inner = inner_maker(coef, lanes)

    def second(i, carry):
        ps = [s[0, i, j] for j in range(NP)]
        dp, du = along_middle(ps, [s[2, i, j] for j in range(NP)], lanes)
        for j in range(NP):
            dq, dw = inner(ps[j], s[3, i, j])
            r[0, i, j] = r[0, i, j] + (dp[j] + dq)
            r[2, i, j] = du[j] if forcing is None else forcing[1, i, j] + du[j]
            r[3, i, j] = dw if forcing is None else forcing[2, i, j] + dw
        return carry

    lax.fori_loop(0, NP, second, 0)


def each(function):
    def body(i, carry):
        function(i)
        return carry

    lax.fori_loop(0, NP, body, 0)


def lifts(s, j, flag, even, odd):
    low_core = flag[1] == 0
    from_low = jnp.where(low_core, odd[j], even[j])
    from_high = jnp.where(low_core, even[j], odd[j])
    low = LIFT * (from_low - (s[1, 0, j] + s[0, 0, j]))
    high = LIFT * (from_high - (s[1, NP - 1, j] - s[0, NP - 1, j]))
    return low, high


def put_ends(flag, up, down, even, odd):
    low_core = flag[1] == 0
    even[...] = jnp.where(low_core, up, down)
    odd[...] = jnp.where(low_core, down, up)


def ends_body(flag, w, even, odd):
    put_ends(flag, w[0, NP - 1] + w[1, NP - 1], w[1, 0] - w[0, 0], even, odd)


def inner_body(w, coef, r):
    local_rate(w, r, coef)


def unpack_body(arrived, f, wide):
    groups = f.shape[0] // 128
    stride = groups * CAP + 1
    devices = arrived.shape[0] // stride
    elements = f.shape[-1]
    labels = arrived[pl.ds(stride - 1, devices, stride=stride), :].T
    row = lax.broadcasted_iota(jnp.int32, (elements, devices), 0).astype(F32)
    pick = jnp.concatenate(
        [(row == labels[s : s + 1] - 1.0).astype(F32).astype(BF16) for s in range(CAP)], axis=1
    )
    for g in range(groups):
        for s in range(CAP):
            part = arrived[pl.ds(CAP * g + s, devices, stride=stride), :]
            high, low = halves(part)
            wide[g % 2, s * devices : (s + 1) * devices, 0:128] = high
            wide[g % 2, s * devices : (s + 1) * devices, 128:256] = low
        both = dot(pick, wide[g % 2])
        f[g * 128 : (g + 1) * 128, :] = (both[:, :128] + both[:, 128:]).T


def first_stage_body(flag, w, r0, f, q_even, q_odd, coef, s1, even, odd):
    lanes = w.shape[-1]

    def add(i):
        for k in range(4):
            rate = r0[k, i] if k == 0 else r0[k, i] + f[k - 1, i]
            s1[k, i] = w[k, i] + DT_WAVE * rate

    each(add)

    def lift(j):
        low, high = lifts(w, j, flag, q_even, q_odd)
        low, high = DT_WAVE * low, DT_WAVE * high
        last = NP - 1
        s1[0, 0, j] = s1[0, 0, j] + low
        s1[1, 0, j] = s1[1, 0, j] + low
        s1[0, last, j] = s1[0, last, j] - high
        s1[1, last, j] = s1[1, last, j] + high

    each(lift)
    inner = inner_maker(coef, lanes)
    low_core = flag[1] == 0
    now, then = [], []
    for i, sign in ((NP - 1, 1.0), (0, -1.0)):
        ps = [s1[0, i, j] for j in range(NP)]
        dp, _ = along_middle(ps, [s1[2, i, j] for j in range(NP)], lanes)
        now_rows, then_rows = [], []
        for j in range(NP):
            dq, _ = inner(ps[j], s1[3, i, j], want_u=False)
            rate_p = dp[j] + dq
            rate_u = f[0, i, j]
            for m in range(NP):
                c = float(MATRIX[i, m])
                if c != 0.0:
                    rate_p = rate_p - c * s1[1, m, j]
                    rate_u = rate_u - c * s1[0, m, j]
            u = s1[1, i, j]
            next_p = 0.75 * w[0, i, j] + 0.25 * (ps[j] + DT_WAVE * rate_p)
            next_u = 0.75 * w[1, i, j] + 0.25 * (u + DT_WAVE * rate_u)
            now_rows.append(u + sign * ps[j])
            then_rows.append(next_u + sign * next_p)
        now.append(now_rows)
        then.append(then_rows)
    for j in range(NP):
        for slot, (up, down) in enumerate((now, then)):
            even[slot, j] = jnp.where(low_core, up[j], down[j])
            odd[slot, j] = jnp.where(low_core, down[j], up[j])


def middle_stage_body(w, s1, f, coef, s2, r2, r1):
    local_rate(s1, r1, coef, f)

    def add(i):
        for k in range(4):
            s2[k, i] = 0.75 * w[k, i] + 0.25 * (s1[k, i] + DT_WAVE * r1[k, i])

    each(add)
    local_rate(s2, r2, coef, f)


def last_stage_body(flag, w, s1, s2, r2, q_even, q_odd, coef, out, even, odd, s, r):
    lanes = w.shape[-1]
    last = NP - 1

    def first(j):
        low, high = lifts(s1, j, flag, q_even.at[0], q_odd.at[0])
        low, high = (0.25 * DT_WAVE) * low, (0.25 * DT_WAVE) * high
        s[0, j] = low
        s[1, j] = -high
        new = (s2[0, 0, j] + low, s2[1, 0, j] + low, s2[0, last, j] - high, s2[1, last, j] + high)
        low_core = flag[1] == 0
        from_low = jnp.where(low_core, q_odd[1, j], q_even[1, j])
        from_high = jnp.where(low_core, q_even[1, j], q_odd[1, j])
        lift_low = LIFT * (from_low - (new[1] + new[0]))
        lift_high = LIFT * (from_high - (new[3] - new[2]))
        for i in range(NP):
            a, b = float(MATRIX[i, 0]), float(MATRIX[i, last])
            p = r2[0, i, j] - a * low - b * high
            u = r2[1, i, j] - a * low + b * high
            if i == 0:
                p, u = p + lift_low, u + lift_low
            if i == last:
                p, u = p - lift_high, u + lift_high
            r[0, i, j] = p
            r[1, i, j] = u

    each(first)
    third = 1.0 / 3.0

    def close(k, i, j, state, rate):
        out[k, i, j] = w[k, i, j] * third + (2.0 * third) * (state + DT_WAVE * rate)

    def inside(i, carry):
        for j in range(NP):
            for k in range(4):
                rate = r[k, i, j] if k < 2 else r2[k, i, j]
                close(k, i, j, s2[k, i, j], rate)
        return carry

    lax.fori_loop(1, last, inside, 0)
    inner = inner_maker(coef, lanes)
    for side, i in ((0, 0), (1, last)):
        ps = [s[side, j] for j in range(NP)]
        dp, du = along_middle(ps, None, lanes)
        for j in range(NP):
            dq, dw = inner(ps[j], None)
            rate = r[0, i, j] + dq
            if dp[j] is not None:
                rate = rate + dp[j]
            close(0, i, j, s2[0, i, j] + ps[j], rate)
            change = ps[j] if side == 0 else -ps[j]
            close(1, i, j, s2[1, i, j] + change, r[1, i, j])
            close(2, i, j, s2[2, i, j], r2[2, i, j] + du[j])
            close(3, i, j, s2[3, i, j], r2[3, i, j] + dw)
    put_ends(flag, out[0, last] + out[1, last], out[1, 0] - out[0, 0], even, odd)


def trade(value, axis, odd):
    size = lax.axis_size(axis)
    pairs = []
    for i in range(odd, size + odd, 2):
        a, b = i % size, (i + 1) % size
        pairs += [(a, b), (b, a)]
    return lax.ppermute(value, axis, pairs)


def exchange_all(value):
    return lax.all_to_all(value, AXES, split_axis=0, concat_axis=0, tiled=True)


def advance(density, velocity, pressure, wave, tables, margin_element, margin_block, margin_table):
    planes, rows, width = density.shape
    lanes = wave.shape[-1]
    devices = lax.axis_size("flow") * lax.axis_size("group")
    kinds, nodes = tables.shape[:2]
    stride = 3 * CAP * nodes // 128 + 1
    blocks = planes * rows * width // nodes

    coef = np.stack([MATRIX[np.arange(NP), (np.arange(NP) + k) % NP] for k in range(NP)])
    coef = jnp.asarray(np.broadcast_to(coef[:, :, None], (NP, NP, lanes)).copy())
    odd_flow = lax.axis_index("flow") & 1
    flag = jnp.stack([odd_flow, lax.axis_index("group")]).astype(jnp.int32)
    first_flag = jnp.zeros((2,), jnp.int32)

    inward = (planes - 1) * (1 - odd_flow)
    v_even = trade(lax.dynamic_slice_in_dim(velocity, inward, 1, 1), "flow", 0)
    v_odd = trade(lax.dynamic_slice_in_dim(velocity, planes - 1 - inward, 1, 1), "flow", 1)
    v_part = trade(velocity, "group", 0)

    block = sds(5, planes, rows, width)
    fields = call(fields_body, block, 1_000_000, limit=WHOLE_VMEM)(density, velocity, pressure)

    def surround(own):
        even = trade(own, "flow", 0)
        return (own, even, trade(own, "flow", 1))

    def swap_rows(pieces):
        return [trade(p, "group", 0) for p in pieces]

    pieces = surround(fields)
    others = swap_rows(pieces)

    select, labels = call(
        lambda *refs: slots_body(*refs, blocks=blocks),
        (sds(CAP * devices, 256, dtype=BF16), sds(devices, 128)),
        1_000_000,
        limit=WHOLE_VMEM,
    )(margin_element, margin_block, margin_table)

    pack = call(
        pack_body,
        sds(devices * stride, 128),
        8_000_000,
        scratch=(
            pltpu.VMEM((2, 3 * planes * rows, 128), F32),
            pltpu.VMEM((3, 256, nodes), BF16),
            pltpu.VMEM(tables.shape, F32),
            pltpu.VMEM((devices * stride, 128), F32),
            pltpu.SemaphoreType.DMA((kinds + 2,)),
        ),
        specs="svvvvhvv",
        limit=WHOLE_VMEM,
        out_specs="h",
    )

    def send(which, *speeds):
        sent = pack(which, *speeds, tables, select, labels)
        sent = exchange_all(sent.reshape(devices, 1, stride * 128))
        return sent.reshape(devices * stride, 128)

    arrived_1 = send(flag, velocity, v_part, v_even, v_odd)

    speed = sds(3, planes, rows, width)
    thin = sds(3, 1, rows, width)
    wide = pltpu.VMEM((5, 3 * planes, 2 * rows, width), F32)
    new_own, new_part, own, part, low, high = call(
        first_flow_body,
        (block, block, speed, speed, thin, thin),
        60_000_000,
        scratch=[wide] * 4,
        specs="s" + 6 * "v",
    )(flag, *pieces, *others)
    arrived_2 = send(first_flag, own, part, high, low)
    pieces = surround(new_own)

    def finish_flow(pieces):
        return call(
            last_flow_body, block, 30_000_000, scratch=[wide] * 4, specs="s" + 6 * "v"
        )(flag, *pieces, new_part, *swap_rows(pieces[1:]))

    state = sds(*wave.shape)
    hold = pltpu.VMEM(wave.shape, F32)
    face = sds(NP, NP, lanes)
    pair = sds(2, NP, NP, lanes)
    inner = call(inner_body, state, 8_000_000)
    unpack = call(
        unpack_body,
        sds(3 * nodes, lanes),
        8_000_000,
        scratch=[pltpu.VMEM((2, CAP * devices, 256), BF16)],
    )
    first_stage = call(first_stage_body, (state, pair, pair), 4_000_000, specs="svvvvvv")
    middle_stage = call(middle_stage_body, (state, state), 16_000_000, scratch=[hold])
    last_stage = call(
        last_stage_body,
        (state, face, face),
        6_000_000,
        scratch=[pltpu.VMEM((2, NP, NP, lanes), F32), pltpu.VMEM((2,) + wave.shape[1:], F32)],
        specs="svvvvvvv",
    )

    def around(even, odd):
        return (trade(even, "group", 0), trade(odd, AXES, 1))

    ends = call(ends_body, (face, face), 100_000, specs="sv")(flag, wave)
    for turn, arrived in enumerate((arrived_1, arrived_2)):
        faces = around(*ends)
        rate = inner(wave, coef)
        forcing = unpack(arrived).reshape(3, *wave.shape[1:])
        s1, *ends = first_stage(flag, wave, rate, forcing, *faces, coef)
        faces = around(*ends)
        if turn == 0:
            pieces, _ = lax.optimization_barrier((pieces, ends))
            flow_state = finish_flow(pieces)
        s2, r2 = middle_stage(wave, s1, forcing, coef)
        wave, *ends = last_stage(flag, wave, s1, s2, r2, *faces, coef)
    return (flow_state, wave, forcing)


def solution(mesh):
    in_specs = (
        P("flow", "group", None),
        P(None, "flow", "group", None),
        P("flow", "group", None),
        P(None, None, None, None, AXES),
        P(),
        P(AXES, None),
        P(AXES, None),
        P(AXES, None),
    )
    out_specs = (
        P(None, "flow", "group", None),
        P(None, None, None, None, AXES),
        P(None, None, None, None, AXES),
    )
    return jax.shard_map(advance, mesh=mesh, in_specs=in_specs, out_specs=out_specs, check_vma=False)
```

```python
import jax
import jax.numpy as jnp
import numpy as np
from jax import lax
from jax.experimental import pallas as pl
from jax.experimental.pallas import tpu as pltpu
from jax.sharding import PartitionSpec as P


NP = 8
EZ = 16
CAP = 4
GAMMA = 1.4
DT_FLOW = 0.08
DT_WAVE = 0.01
F32 = jnp.float32
BF16 = jnp.bfloat16
AXES = ("flow", "group")
VMEM_LIMIT = 26 * 2**20
WHOLE_VMEM = 58 * 2**20


def legendre_pair(nodes, degree):
    previous = np.ones(nodes.shape[0])
    current = nodes * 1.0
    for order in range(2, degree + 1):
        previous, current = (
            current,
            ((2 * order - 1) * nodes * current - (order - 1) * previous) / order,
        )
    return (previous, current)


def lobatto(point_count):
    degree = point_count - 1
    nodes = -np.cos(np.pi * np.arange(point_count) / degree)
    for _ in range(60):
        previous, current = legendre_pair(nodes, degree)
        nodes = nodes - (nodes * current - previous) / (point_count * current)
    previous, values = legendre_pair(nodes, degree)
    weights = 2.0 / (degree * (degree + 1) * values**2)
    identity = np.eye(point_count)
    differ = nodes[:, None] - nodes[None, :] + identity
    matrix = values[:, None] / values[None, :] / differ * (1.0 - identity)
    matrix[0, 0] = -degree * (degree + 1) / 4.0
    matrix[-1, -1] = degree * (degree + 1) / 4.0
    return (matrix.astype(np.float32), float(weights[0]))


MATRIX, END_WEIGHT = lobatto(NP)
LIFT = 0.5 / END_WEIGHT


def sds(*shape, dtype=F32):
    return jax.ShapeDtypeStruct(shape, dtype)


def call(body, out_shape, flops, scratch=(), specs=None, out_specs=None, limit=VMEM_LIMIT):
    kinds = {"s": pltpu.SMEM, "v": pltpu.VMEM, "h": pltpu.HBM}
    extra = {}
    if specs is not None:
        extra["in_specs"] = [pl.BlockSpec(memory_space=kinds[k]) for k in specs]
    if out_specs is not None:
        extra["out_specs"] = pl.BlockSpec(memory_space=kinds[out_specs])
    return pl.pallas_call(
        body,
        out_shape=out_shape,
        scratch_shapes=list(scratch),
        cost_estimate=pl.CostEstimate(flops=flops, bytes_accessed=4_000_000, transcendentals=0),
        compiler_params=pltpu.CompilerParams(vmem_limit_bytes=limit),
        **extra,
    )


def flags():
    return lax.axis_index("flow") & 1, lax.axis_index("group")


def halves(value):
    high = value.astype(BF16)
    return high, (value - high.astype(F32)).astype(BF16)


def dot(left, right, dims=((1,), (0,))):
    return lax.dot_general(left, right, (dims, ((), ())), preferred_element_type=F32)


def fields_body(rho_ref, vel_ref, pre_ref, f_ref):
    rho = rho_ref[...]
    v = [vel_ref[d] for d in range(3)]
    kinetic = v[0] * v[0] + v[1] * v[1] + v[2] * v[2]
    f_ref[0] = rho
    for d in range(3):
        f_ref[1 + d] = rho * v[d]
    f_ref[4] = pre_ref[...] / (GAMMA - 1.0) + 0.5 * rho * kinetic


def slots_body(me_ref, mb_ref, mt_ref, sel_ref, lab_ref, *, blocks):
    entries = me_ref.shape[1]
    devices = lab_ref.shape[0]
    shape = (devices, entries)
    owner = me_ref[...] >> 7
    place = (me_ref[...] & 127).astype(F32)
    lane = lax.broadcasted_iota(jnp.int32, shape, 0)
    owned = (lane == owner).astype(F32)
    before = lax.broadcasted_iota(jnp.int32, (entries, entries), 0) < lax.broadcasted_iota(
        jnp.int32, (entries, entries), 1
    )
    ahead = dot(owned.astype(BF16), before.astype(F32).astype(BF16))
    rank = jnp.sum(owned * ahead, axis=0, keepdims=True)
    combo = (lane == mt_ref[...] * blocks + mb_ref[...]).astype(F32).astype(BF16)
    for s in range(CAP):
        mine = jnp.where(rank == float(s), owned, 0.0).astype(BF16)
        pick = dot(mine, combo, ((1,), (1,))).astype(BF16)
        half = devices // 2
        for h in range(2):
            at = (h * CAP + s) * half
            for side in range(2):
                sel_ref[at : at + half, side * 128 : (side + 1) * 128] = pick[
                    h * half : (h + 1) * half
                ]
    spread = jnp.where(lane.astype(F32) == rank, place + 1.0, 0.0).astype(BF16)
    lab_ref[...] = dot(owned.astype(BF16), spread, ((1,), (1,)))


def pack_body(
    own_ref,
    part_ref,
    even_ref,
    odd_ref,
    tab_hbm,
    sel_ref,
    lab_ref,
    out_hbm,
    src,
    mp,
    tab,
    out,
    sems,
    *,
    paired,
):
    planes, rows, width = own_ref.shape[1:]
    tables, nodes = tab.shape[0], tab.shape[1]
    blocks = 128 // tables
    loads = [pltpu.make_async_copy(tab_hbm.at[t], tab.at[t], sems.at[t]) for t in range(tables)]
    for load in loads:
        load.start()
    low_flow = flags()[0] == 0

    def pick(when, other):
        return jnp.where(low_flow, when, other) if paired else when

    def turn(value, by):
        return pltpu.roll(value, by % width, 1)

    for x in range(planes):
        v = [own_ref[d, x] for d in range(3)]

        def along_x(d):
            if x == 0:
                below = pick(odd_ref[d, 0], even_ref[d, 0])
            else:
                below = own_ref[d, x - 1]
            if x == planes - 1:
                above = pick(even_ref[d, 0], odd_ref[d, 0])
            else:
                above = own_ref[d, x + 1]
            return 0.5 * (above - below)

        def along_y(d):
            both = jnp.concatenate([v[d], part_ref[d, x]], axis=0)
            up = pltpu.roll(both, 2 * rows - 1, 0)[:rows]
            down = pltpu.roll(both, 1, 0)[:rows]
            return 0.5 * (up - down)

        def along_z(d):
            return 0.5 * (turn(v[d], -1) - turn(v[d], 1))

        curl = (
            along_y(2) - along_z(1),
            along_z(0) - along_x(2),
            along_x(1) - along_y(0),
        )
        for c in range(3):
            a, b = (c + 1) % 3, (c + 2) % 3
            base = (c * planes + x) * rows
            lamb = curl[a] * v[b] - curl[b] * v[a]
            src[0, base : base + rows, :] = lamb[:, :128]
            src[1, base : base + rows, :] = lamb[:, 128:]
    count = 3 * blocks
    split = [
        halves(src[half, pl.ds(start, count, stride=2), :])
        for start in range(2)
        for half in range(2)
    ]
    left = jnp.concatenate(
        [
            jnp.concatenate([h for h, _ in split], axis=1),
            jnp.concatenate([l for _, l in split], axis=1),
        ],
        axis=0,
    )
    for t in range(tables):
        loads[t].wait()
        high, low = halves(tab[t])
        wide = dot(left, high)
        mapped = wide[:count] + wide[count:] + dot(left[:count], low)
        for c in range(3):
            high, low = halves(mapped[c * blocks : (c + 1) * blocks])
            mp[c, t * blocks : (t + 1) * blocks, :] = high
            mp[c, 128 + t * blocks : 128 + (t + 1) * blocks, :] = low
    devices = lab_ref.shape[0]
    half = devices // 2
    groups = nodes // 128
    stride = 3 * groups * CAP + 1
    out[pl.ds(stride - 1, devices, stride=stride), :] = lab_ref[...]
    stores = []
    for h in range(2):
        for c in range(3):
            filled = dot(sel_ref[h * CAP * half : (h + 1) * CAP * half, :], mp[c])
            for s in range(CAP):
                for m in range(groups):
                    row = h * half * stride + CAP * (c * groups + m) + s
                    out[pl.ds(row, half, stride=stride), :] = filled[
                        s * half : (s + 1) * half, m * 128 : (m + 1) * 128
                    ]
        part = pl.ds(h * half * stride, half * stride)
        store = pltpu.make_async_copy(out.at[part], out_hbm.at[part], sems.at[tables + h])
        store.start()
        stores.append(store)
    for store in stores:
        store.wait()


def primitives(s):
    inverse = 1.0 / s[0]
    v = [s[1 + d] * inverse for d in range(3)]
    kinetic = v[0] * v[0] + v[1] * v[1] + v[2] * v[2]
    p = (GAMMA - 1.0) * (s[4] - 0.5 * s[0] * kinetic)
    return v, p, jnp.sqrt(GAMMA * p * inverse)


def flux_of(s, v, p, d, k):
    if k == 0:
        return s[1 + d]
    if k == 4:
        return (s[4] + p) * v
    product = s[k] * v
    return product + p if k == 1 + d else product


def flow_stage(src, base, dst, prim, first, last, weights, shift=0, rows=None):
    a_weight, b_weight = weights

    def prepare(x, carry):
        v, p, sound = primitives([src[k, x] for k in range(5)])
        for d in range(3):
            prim[d, x] = v[d]
        prim[3, x] = p
        prim[4, x] = sound
        return carry

    lax.fori_loop(first - 1, last + 1, prepare, 0)

    def advance(x, carry):
        s = [src[k, x] for k in range(5)]
        total = []
        sound = prim[4, x]
        p = prim[3, x]
        up = [src[k, x + 1] for k in range(5)]
        down = [src[k, x - 1] for k in range(5)]
        v, vu, vd = prim[0, x], prim[0, x + 1], prim[0, x - 1]
        speed = jnp.abs(v) + sound
        fast_u = jnp.maximum(speed, jnp.abs(vu) + prim[4, x + 1])
        fast_d = jnp.maximum(speed, jnp.abs(vd) + prim[4, x - 1])
        pu, pd = prim[3, x + 1], prim[3, x - 1]
        for k in range(5):
            jump = fast_u * (up[k] - s[k]) - fast_d * (s[k] - down[k])
            total.append(flux_of(up, vu, pu, 0, k) - flux_of(down, vd, pd, 0, k) - jump)
        for d, axis in ((1, 0), (2, 1)):
            size = s[0].shape[axis]
            v = prim[d, x]
            speed = jnp.abs(v) + sound
            fast = jnp.maximum(speed, pltpu.roll(speed, size - 1, axis))
            for k in range(5):
                flux = flux_of(s, v, p, d, k)
                face = flux + pltpu.roll(flux, size - 1, axis)
                face = face - fast * (pltpu.roll(s[k], size - 1, axis) - s[k])
                total[k] = total[k] + (face - pltpu.roll(face, 1, axis))
        for k in range(5):
            value = b_weight * s[k] - (0.5 * DT_FLOW * b_weight) * total[k]
            if a_weight is not None:
                value = value + a_weight * base[k, x]
            if rows is not None:
                value = value[:rows]
            dst[k, x - shift] = value
        return carry

    lax.fori_loop(first, last, advance, 0)


STAGES = ((None, 1.0), (0.75, 0.25), (1.0 / 3.0, 2.0 / 3.0))


def place(s0, start, mine, other, first=0):
    rows = mine.shape[2]
    for i in range(mine.shape[1]):
        for k in range(5):
            s0[k, start + first + i, :rows] = mine[k, i]
            s0[k, start + first + i, rows:] = other[k, i]


def around_own(planes):
    above = jnp.where(flags()[0] == 0, 2 * planes, 0)
    return above, 2 * planes - above


def first_flow_body(*refs):
    mine, other = refs[:3], refs[3:6]
    new_own, new_part, mid, low, high = refs[6:11]
    own_ref, part_ref, lo_ref, hi_ref = refs[11:15]
    s0, s1, s2, prim = refs[15:]
    planes, rows = mine[0].shape[1], mine[0].shape[2]
    for start, a, b in zip((planes, *around_own(planes)), mine, other):
        place(s0, start, a, b)
    wide = 3 * planes
    flow_stage(s0, None, s1, prim, 1, wide - 1, STAGES[0])
    flow_stage(s1, s0, s2, prim, 2, wide - 2, STAGES[1])
    flow_stage(s2, s0, s1, prim, 3, wide - 3, STAGES[2])
    for i in range(-1, planes + 1):
        x = planes + i
        inverse = 1.0 / s1[0, x]
        v = [s1[1 + d, x] * inverse for d in range(3)]
        for d in range(3):
            if i == -1:
                lo_ref[d, 0] = v[d][:rows]
            elif i == planes:
                hi_ref[d, 0] = v[d][:rows]
            else:
                own_ref[d, i] = v[d][:rows]
                part_ref[d, i] = v[d][rows:]
        for k in range(5):
            if i == -1:
                low[k, 0] = s1[k, x]
            elif i == planes:
                high[k, 0] = s1[k, x]
            else:
                new_own[k, i] = s1[k, x, :rows]
                new_part[k, i] = s1[k, x, rows:]
                if 0 < i < planes - 1:
                    mid[k, i - 1] = s1[k, x, :rows]


def last_flow_body(*refs):
    own, part, low, high = refs[:4]
    even, odd, even_part, odd_part, out_ref = refs[4:9]
    s0, s1, s2, prim = refs[9:]
    planes, rows = own.shape[1], own.shape[2]
    place(s0, planes, own, part)
    even_at, odd_at = around_own(planes)
    place(s0, even_at, even, even_part, first=1)
    place(s0, odd_at, odd, odd_part, first=1)
    wide = 3 * planes
    for k in range(5):
        s0[k, planes - 1] = low[k, 0]
        s0[k, 2 * planes] = high[k, 0]
    flow_stage(s0, None, s1, prim, 2, wide - 2, STAGES[0])
    flow_stage(s1, s0, s2, prim, 3, wide - 3, STAGES[1])
    flow_stage(s2, s0, out_ref, prim, planes, 2 * planes, STAGES[2], shift=planes, rows=rows)


def derive(values):
    half = NP // 2
    even = [values[i] + values[NP - 1 - i] for i in range(half)]
    odd = [values[i] - values[NP - 1 - i] for i in range(half)]
    tops, bottoms = [], []
    for a in range(half):
        plus = minus = None
        for i in range(half):
            ce = 0.5 * float(MATRIX[a, i] + MATRIX[a, NP - 1 - i])
            co = 0.5 * float(MATRIX[a, i] - MATRIX[a, NP - 1 - i])
            te, to = ce * even[i], co * odd[i]
            plus = te if plus is None else plus + te
            minus = to if minus is None else minus + to
        tops.append(plus + minus)
        bottoms.append(minus - plus)
    return tops + bottoms[::-1]


def along_middle(ps, us, lanes):
    p = derive(ps)
    below, above = (ps[-1], -ps[0]) if us is None else (ps[-1] + us[-1], us[0] - ps[0])
    own_low, own_high = (ps[0], -ps[-1]) if us is None else (ps[0] + us[0], us[-1] - ps[-1])
    low = LIFT * (pltpu.roll(below, EZ, 1) - own_low)
    high = LIFT * (pltpu.roll(above, lanes - EZ, 1) - own_high)
    dp = [None] * NP if us is None else [-u for u in derive(us)]
    du = [-value for value in p]
    dp[0] = low if dp[0] is None else dp[0] + low
    dp[-1] = -high if dp[-1] is None else dp[-1] - high
    du[0] = du[0] + low
    du[-1] = du[-1] + high
    return dp, du


def inner_maker(coef, lanes):
    lane = lax.broadcasted_iota(jnp.int32, (NP, lanes), 1)
    row = lax.broadcasted_iota(jnp.int32, (NP, lanes), 0)
    firsts = (lane & (EZ - 1)) == 0
    lasts = (lane & (EZ - 1)) == EZ - 1
    is_low = row == 0
    lift_u = jnp.where(is_low | (row == NP - 1), LIFT, 0.0)
    lift_p = jnp.where(is_low, LIFT, jnp.where(row == NP - 1, -LIFT, 0.0))

    def slope(value):
        total = coef[0] * value
        for k in range(1, NP):
            total = total + coef[k] * pltpu.roll(value, NP - k, 0)
        return total

    def jump_of(p, u):
        up, down = (p, -p) if u is None else (u + p, u - p)
        edge = jnp.where(is_low, pltpu.roll(up, 1, 0), pltpu.roll(down, NP - 1, 0))
        from_low = jnp.where(firsts, pltpu.roll(edge, lanes + 1 - EZ, 1), pltpu.roll(edge, 1, 1))
        from_high = jnp.where(
            lasts, pltpu.roll(edge, EZ - 1, 1), pltpu.roll(edge, lanes - 1, 1)
        )
        return jnp.where(is_low, from_low - up, from_high - down)

    def both(p, u, want_u=True):
        jump = jump_of(p, u)
        dp = lift_p * jump if u is None else lift_p * jump - slope(u)
        return dp, (lift_u * jump - slope(p)) if want_u else None

    return both


def local_rate(s, r, coef, forcing=None):
    lanes = s.shape[-1]

    def first(j, carry):
        p = derive([s[0, i, j] for i in range(NP)])
        u = derive([s[1, i, j] for i in range(NP)])
        for i in range(NP):
            r[0, i, j] = -u[i]
            r[1, i, j] = -p[i] if forcing is None else forcing[0, i, j] - p[i]
        return carry

    lax.fori_loop(0, NP, first, 0)
    inner = inner_maker(coef, lanes)

    def second(i, carry):
        ps = [s[0, i, j] for j in range(NP)]
        dp, du = along_middle(ps, [s[2, i, j] for j in range(NP)], lanes)
        for j in range(NP):
            dq, dw = inner(ps[j], s[3, i, j])
            r[0, i, j] = r[0, i, j] + (dp[j] + dq)
            r[2, i, j] = du[j] if forcing is None else forcing[1, i, j] + du[j]
            r[3, i, j] = dw if forcing is None else forcing[2, i, j] + dw
        return carry

    lax.fori_loop(0, NP, second, 0)


def each(function):
    def body(i, carry):
        function(i)
        return carry

    lax.fori_loop(0, NP, body, 0)


LAST = NP - 1


def chosen(low, when_low, when_high):
    return jnp.where(low, when_low, when_high)


def add_lifts(s, r, incoming=None):
    def lift(j):
        from_low, from_high = (0.0, 0.0) if incoming is None else incoming(j)
        low = LIFT * (from_low - (s[1, 0, j] + s[0, 0, j]))
        high = LIFT * (from_high - (s[1, LAST, j] - s[0, LAST, j]))
        r[0, 0, j] = r[0, 0, j] + low
        r[1, 0, j] = r[1, 0, j] + low
        r[0, LAST, j] = r[0, LAST, j] - high
        r[1, LAST, j] = r[1, LAST, j] + high

    each(lift)


def ends_body(w, even, odd):
    low_core = flags()[1] == 0
    up, down = w[0, LAST] + w[1, LAST], w[1, 0] - w[0, 0]
    even[...] = chosen(low_core, up, down)
    odd[...] = chosen(low_core, down, up)


def rate_body(w, even, odd, coef, r):
    low_core = flags()[1] == 0
    local_rate(w, r, coef)
    add_lifts(
        w,
        r,
        lambda j: (
            chosen(low_core, odd[j], even[j]),
            chosen(low_core, even[j], odd[j]),
        ),
    )


def unpack_body(w, r0, arrived_hbm, coef, f, s1, even, odd, arrived, wide, sums, sems):
    lanes = w.shape[-1]
    groups = sums.shape[0]
    stride = groups * CAP + 1
    half = arrived.shape[0] // stride // 2
    loads = []
    for h in range(2):
        part = pl.ds(h * half * stride, half * stride)
        loads.append(pltpu.make_async_copy(arrived_hbm.at[part], arrived.at[part], sems.at[h]))
        loads[-1].start()
    row = lax.broadcasted_iota(jnp.int32, (lanes, half), 0).astype(F32)
    for h in range(2):
        loads[h].wait()
        base = h * half * stride
        labels = arrived[pl.ds(base + stride - 1, half, stride=stride), :].T
        pick = jnp.concatenate(
            [(row == labels[s : s + 1] - 1.0).astype(F32).astype(BF16) for s in range(CAP)],
            axis=1,
        )
        for g in range(groups):
            for s in range(CAP):
                part = arrived[pl.ds(base + CAP * g + s, half, stride=stride), :]
                high, low = halves(part)
                wide[g % 2, s * half : (s + 1) * half, 0:128] = high
                wide[g % 2, s * half : (s + 1) * half, 128:256] = low
            both = dot(pick, wide[g % 2])
            if h == 0:
                sums[g] = both
                continue
            both = both + sums[g]
            nodes = (both[:, :128] + both[:, 128:]).T
            for row_of in range(128 // NP):
                at = g * 128 // NP + row_of
                c, i, j = at // (NP * NP), at // NP % NP, at % NP
                f[c, i, j] = nodes[row_of * NP : (row_of + 1) * NP, :]

    def add(i):
        for k in range(4):
            rate = r0[k, i] if k == 0 else r0[k, i] + f[k - 1, i]
            s1[k, i] = w[k, i] + DT_WAVE * rate

    each(add)
    inner = inner_maker(coef, lanes)
    low_core = flags()[1] == 0
    now, then = [], []
    for i, sign in ((LAST, 1.0), (0, -1.0)):
        ps = [s1[0, i, j] for j in range(NP)]
        dp, _ = along_middle(ps, [s1[2, i, j] for j in range(NP)], lanes)
        now_rows, then_rows = [], []
        for j in range(NP):
            dq, _ = inner(ps[j], s1[3, i, j], want_u=False)
            rate_p = dp[j] + dq
            rate_u = f[0, i, j]
            for m in range(NP):
                c = float(MATRIX[i, m])
                if c != 0.0:
                    rate_p = rate_p - c * s1[1, m, j]
                    rate_u = rate_u - c * s1[0, m, j]
            u = s1[1, i, j]
            next_p = 0.75 * w[0, i, j] + 0.25 * (ps[j] + DT_WAVE * rate_p)
            next_u = 0.75 * w[1, i, j] + 0.25 * (u + DT_WAVE * rate_u)
            now_rows.append(u + sign * ps[j])
            then_rows.append(next_u + sign * next_p)
        now.append(now_rows)
        then.append(then_rows)
    for j in range(NP):
        for slot, (up, down) in enumerate((now, then)):
            even[slot, j] = chosen(low_core, up[j], down[j])
            odd[slot, j] = chosen(low_core, down[j], up[j])


def middle_body(w, s1, f, coef, s2, r2, r1):
    local_rate(s1, r1, coef, f)
    add_lifts(s1, r1)

    def add(i):
        for k in range(4):
            s2[k, i] = 0.75 * w[k, i] + 0.25 * (s1[k, i] + DT_WAVE * r1[k, i])

    each(add)
    local_rate(s2, r2, coef, f)
    add_lifts(s2, r2)


def relay_body(w, s1, f, coef, even, odd, s2, r2, even3, odd3, far_even, far_odd, r1):
    middle_body(w, s1, f, coef, s2, r2, r1)
    low_flow, low_core = flags()[0] == 0, flags()[1] == 0

    def third(k, i, j):
        return w[k, i, j] * (1.0 / 3.0) + (2.0 / 3.0) * (s2[k, i, j] + DT_WAVE * r2[k, i, j])

    def send(j):
        for slot in range(2):
            even3[slot, j] = even[slot, j]
            odd3[slot, j] = odd[slot, j]
        up = third(1, LAST, j) + third(0, LAST, j)
        down = third(1, 0, j) - third(0, 0, j)
        even3[2, j] = chosen(low_core, up, down)
        odd3[2, j] = chosen(low_core, down, up)
        up = chosen(low_core, even[0, j], odd[0, j])
        down = chosen(low_core, odd[0, j], even[0, j])
        far_even[j] = chosen(low_flow, up, down)
        far_odd[j] = chosen(low_flow, down, up)

    each(send)


def close_step(w, s2, r2, even, odd, coef, out, s, r):
    lanes = w.shape[-1]
    low_core = flags()[1] == 0

    def first(j):
        low = (0.25 * DT_WAVE * LIFT) * chosen(low_core, odd[0, j], even[0, j])
        high = (0.25 * DT_WAVE * LIFT) * chosen(low_core, even[0, j], odd[0, j])
        s[0, j] = low
        s[1, j] = -high
        lift_low = LIFT * (chosen(low_core, odd[1, j], even[1, j]) - 2.0 * low)
        lift_high = LIFT * (chosen(low_core, even[1, j], odd[1, j]) - 2.0 * high)
        for i in range(NP):
            a, b = float(MATRIX[i, 0]), float(MATRIX[i, LAST])
            p = r2[0, i, j] - a * low - b * high
            u = r2[1, i, j] - a * low + b * high
            if i == 0:
                p, u = p + lift_low, u + lift_low
            if i == LAST:
                p, u = p - lift_high, u + lift_high
            r[0, i, j] = p
            r[1, i, j] = u

    each(first)
    third = 1.0 / 3.0

    def close(k, i, j, state, rate):
        out[k, i, j] = w[k, i, j] * third + (2.0 * third) * (state + DT_WAVE * rate)

    def inside(i, carry):
        for j in range(NP):
            for k in range(4):
                rate = r[k, i, j] if k < 2 else r2[k, i, j]
                close(k, i, j, s2[k, i, j], rate)
        return carry

    lax.fori_loop(1, LAST, inside, 0)
    inner = inner_maker(coef, lanes)
    for side, i in ((0, 0), (1, LAST)):
        ps = [s[side, j] for j in range(NP)]
        dp, du = along_middle(ps, None, lanes)
        for j in range(NP):
            dq, dw = inner(ps[j], None)
            rate = r[0, i, j] + dq
            if dp[j] is not None:
                rate = rate + dp[j]
            close(0, i, j, s2[0, i, j] + ps[j], rate)
            change = ps[j] if side == 0 else -ps[j]
            close(1, i, j, s2[1, i, j] + change, r[1, i, j])
            close(2, i, j, s2[2, i, j], r2[2, i, j] + du[j])
            close(3, i, j, s2[3, i, j], r2[3, i, j] + dw)


def turn_body(
    w, s2, r2, even, odd, far_even, far_odd, own_even, own_odd, coef, out, r0, s, r, q
):
    close_step(w, s2, r2, even, odd, coef, out, s, r)
    lanes = w.shape[-1]
    low_flow, low_core = flags()[0] == 0, flags()[1] == 0
    inner = inner_maker(coef, lanes)
    weight = 0.25 * DT_WAVE * LIFT

    def spill(values):
        dp, _ = along_middle(values, None, lanes)
        found = []
        for j in range(NP):
            dq, _ = inner(values[j], None, want_u=False)
            found.append(dq if dp[j] is None else dp[j] + dq)
        return found

    ups = [weight * chosen(low_core, own_even[0, j], own_odd[0, j]) for j in range(NP)]
    downs = [weight * chosen(low_core, own_odd[0, j], own_even[0, j]) for j in range(NP)]
    step = 2.0 / 3.0 * DT_WAVE
    for j, (a, b) in enumerate(zip(spill([-d for d in downs]), spill(ups))):
        far_low = chosen(low_flow, far_odd[j], far_even[j])
        far_high = chosen(low_flow, far_even[j], far_odd[j])
        a = a - (2.0 * float(MATRIX[LAST, 0]) * weight) * far_low
        b = (2.0 * float(MATRIX[0, LAST]) * weight) * far_high - b
        q[0, j] = chosen(low_core, odd[2, j], even[2, j]) + step * a
        q[1, j] = chosen(low_core, even[2, j], odd[2, j]) + step * b
    local_rate(out, r0, coef)
    add_lifts(out, r0, lambda j: (q[0, j], q[1, j]))


def trade(value, axis, odd):
    size = lax.axis_size(axis)
    pairs = []
    for i in range(odd, size + odd, 2):
        a, b = i % size, (i + 1) % size
        pairs += [(a, b), (b, a)]
    return lax.ppermute(value, axis, pairs)


def exchange_all(value):
    return lax.all_to_all(value, AXES, split_axis=0, concat_axis=0, tiled=True)


def advance(density, velocity, pressure, wave, tables, margin_element, margin_block, margin_table):
    planes, rows, width = density.shape
    lanes = wave.shape[-1]
    devices = lax.axis_size("flow") * lax.axis_size("group")
    kinds, nodes = tables.shape[:2]
    stride = 3 * CAP * nodes // 128 + 1
    blocks = planes * rows * width // nodes

    coef = np.stack([MATRIX[np.arange(NP), (np.arange(NP) + k) % NP] for k in range(NP)])
    coef = jnp.asarray(np.broadcast_to(coef[:, :, None], (NP, NP, lanes)).copy())
    odd_flow = lax.axis_index("flow") & 1

    inward = (planes - 1) * (1 - odd_flow)
    v_even = trade(lax.dynamic_slice_in_dim(velocity, inward, 1, 1), "flow", 0)
    v_odd = trade(lax.dynamic_slice_in_dim(velocity, planes - 1 - inward, 1, 1), "flow", 1)
    v_part = trade(velocity, "group", 0)

    block = sds(5, planes, rows, width)
    fields = call(fields_body, block, 1_000_000, limit=WHOLE_VMEM)(density, velocity, pressure)

    def surround(own):
        even = trade(own, "flow", 0)
        return (own, even, trade(own, "flow", 1))

    def swap_rows(pieces):
        return [trade(p, "group", 0) for p in pieces]

    pieces = surround(fields)
    others = swap_rows(pieces)

    select, labels = call(
        lambda *refs: slots_body(*refs, blocks=blocks),
        (sds(CAP * devices, 256, dtype=BF16), sds(devices, 128)),
        1_000_000,
        limit=WHOLE_VMEM,
    )(margin_element, margin_block, margin_table)

    def send(paired, *speeds):
        sent = call(
            lambda *refs: pack_body(*refs, paired=paired),
            sds(devices * stride, 128),
            8_000_000,
            scratch=(
                pltpu.VMEM((2, 3 * planes * rows, 128), F32),
                pltpu.VMEM((3, 256, nodes), BF16),
                pltpu.VMEM(tables.shape, F32),
                pltpu.VMEM((devices * stride, 128), F32),
                pltpu.SemaphoreType.DMA((kinds + 2,)),
            ),
            specs="vvvvhvv",
            out_specs="h",
            limit=WHOLE_VMEM,
        )(*speeds, tables, select, labels)
        sent = exchange_all(sent.reshape(devices, 1, stride * 128))
        return sent.reshape(devices * stride, 128)

    arrived_1 = send(True, velocity, v_part, v_even, v_odd)

    speed = sds(3, planes, rows, width)
    thin = sds(3, 1, rows, width)
    edge = sds(5, 1, 2 * rows, width)
    wide = pltpu.VMEM((5, 3 * planes, 2 * rows, width), F32)
    new_own, new_part, mid, low_edge, high_edge, own, part, low, high = call(
        first_flow_body,
        (block, block, sds(5, planes - 2, rows, width), edge, edge, speed, speed, thin, thin),
        60_000_000,
        scratch=[wide] * 4,
    )(*pieces, *others)
    arrived_2 = send(False, own, part, high, low)
    mids = surround(mid)[1:]

    def finish_flow(mids):
        return call(last_flow_body, block, 30_000_000, scratch=[wide] * 4)(
            new_own, new_part, low_edge, high_edge, *mids, *swap_rows(mids)
        )

    state = sds(*wave.shape)
    force = sds(3, *wave.shape[1:])
    hold = pltpu.VMEM(wave.shape, F32)
    face = sds(NP, NP, lanes)
    pair = sds(2, NP, NP, lanes)
    triple = sds(3, NP, NP, lanes)
    sides = pltpu.VMEM((2, NP, NP, lanes), F32)
    couple = pltpu.VMEM((2,) + wave.shape[1:], F32)
    unpack = call(
        unpack_body,
        (force, state, pair, pair),
        12_000_000,
        scratch=[
            pltpu.VMEM((devices * stride, 128), F32),
            pltpu.VMEM((2, CAP * devices // 2, 256), BF16),
            pltpu.VMEM((3 * nodes // 128, lanes, 256), F32),
            pltpu.SemaphoreType.DMA((2,)),
        ],
        specs="vvhv",
    )

    def around(even, odd):
        return (trade(even, "group", 0), trade(odd, AXES, 1))

    ends = call(ends_body, (face, face), 100_000)(wave)
    faces = around(*ends)
    rate = call(rate_body, state, 8_000_000)(wave, *faces, coef)
    forcing, s1, *ends = unpack(wave, rate, arrived_1, coef)
    s2, r2, even, odd, far_even, far_odd = call(
        relay_body, (state, state, triple, triple, face, face), 16_000_000, scratch=[hold]
    )(wave, s1, forcing, coef, *ends)
    faces = around(even, odd)
    far = (trade(far_even, "flow", 0), trade(far_odd, "flow", 1))
    mids, _ = lax.optimization_barrier((mids, far_even))
    flow_state = finish_flow(mids)
    wave, rate = call(
        turn_body, (state, state), 14_000_000, scratch=[sides, couple, sides]
    )(wave, s2, r2, *faces, *far, *ends, coef)

    forcing, s1, *ends = unpack(wave, rate, arrived_2, coef)
    faces = around(*ends)
    s2, r2 = call(middle_body, (state, state), 16_000_000, scratch=[hold])(wave, s1, forcing, coef)
    wave = call(close_step, state, 6_000_000, scratch=[sides, couple])(wave, s2, r2, *faces, coef)
    return (flow_state, wave, forcing)


def solution(mesh):
    in_specs = (
        P("flow", "group", None),
        P(None, "flow", "group", None),
        P("flow", "group", None),
        P(None, None, None, None, AXES),
        P(),
        P(AXES, None),
        P(AXES, None),
        P(AXES, None),
    )
    out_specs = (
        P(None, "flow", "group", None),
        P(None, None, None, None, AXES),
        P(None, None, None, None, AXES),
    )
    return jax.shard_map(advance, mesh=mesh, in_specs=in_specs, out_specs=out_specs, check_vma=False)
```

```python
import jax
import jax.numpy as jnp
import numpy as np
from jax import lax
from jax.experimental import pallas as pl
from jax.experimental.pallas import tpu as pltpu
from jax.sharding import PartitionSpec as P


NP = 8
EZ = 16
CAP = 4
GAMMA = 1.4
DT_FLOW = 0.08
DT_WAVE = 0.01
F32 = jnp.float32
BF16 = jnp.bfloat16
AXES = ("flow", "group")
VMEM_LIMIT = 26 * 2**20
WHOLE_VMEM = 63_050_000
PACK_VMEM = 55_000_000


def legendre_pair(nodes, degree):
    previous = np.ones(nodes.shape[0])
    current = nodes * 1.0
    for order in range(2, degree + 1):
        previous, current = (
            current,
            ((2 * order - 1) * nodes * current - (order - 1) * previous) / order,
        )
    return (previous, current)


def lobatto(point_count):
    degree = point_count - 1
    nodes = -np.cos(np.pi * np.arange(point_count) / degree)
    for _ in range(60):
        previous, current = legendre_pair(nodes, degree)
        nodes = nodes - (nodes * current - previous) / (point_count * current)
    previous, values = legendre_pair(nodes, degree)
    weights = 2.0 / (degree * (degree + 1) * values**2)
    identity = np.eye(point_count)
    differ = nodes[:, None] - nodes[None, :] + identity
    matrix = values[:, None] / values[None, :] / differ * (1.0 - identity)
    matrix[0, 0] = -degree * (degree + 1) / 4.0
    matrix[-1, -1] = degree * (degree + 1) / 4.0
    return (matrix.astype(np.float32), float(weights[0]))


MATRIX, END_WEIGHT = lobatto(NP)
LIFT = 0.5 / END_WEIGHT


def sds(*shape, dtype=F32):
    return jax.ShapeDtypeStruct(shape, dtype)


def call(body, out_shape, flops, scratch=(), specs=None, out_specs=None, limit=VMEM_LIMIT):
    kinds = {"s": pltpu.SMEM, "v": pltpu.VMEM, "h": pltpu.HBM}
    extra = {}
    if specs is not None:
        extra["in_specs"] = [pl.BlockSpec(memory_space=kinds[k]) for k in specs]
    if out_specs is not None:
        places = [pl.BlockSpec(memory_space=kinds[k]) for k in out_specs]
        extra["out_specs"] = places if len(places) > 1 else places[0]
    return pl.pallas_call(
        body,
        out_shape=out_shape,
        scratch_shapes=list(scratch),
        cost_estimate=pl.CostEstimate(flops=flops, bytes_accessed=4_000_000, transcendentals=0),
        compiler_params=pltpu.CompilerParams(vmem_limit_bytes=limit),
        **extra,
    )


def flags():
    return lax.axis_index("flow") & 1, lax.axis_index("group")


def halves(value):
    high = value.astype(BF16)
    return high, (value - high.astype(F32)).astype(BF16)


def dot(left, right, dims=((1,), (0,))):
    return lax.dot_general(left, right, (dims, ((), ())), preferred_element_type=F32)


def fields_body(rho_ref, vel_ref, pre_ref, me_ref, mb_ref, mt_ref, f_ref, margin_ref):
    for row, ref in enumerate((me_ref, mb_ref, mt_ref)):
        margin_ref[row : row + 1, :] = ref[...]
    rho = rho_ref[...]
    v = [vel_ref[d] for d in range(3)]
    kinetic = v[0] * v[0] + v[1] * v[1] + v[2] * v[2]
    f_ref[0] = rho
    for d in range(3):
        f_ref[1 + d] = rho * v[d]
    f_ref[4] = pre_ref[...] / (GAMMA - 1.0) + 0.5 * rho * kinetic


def slots_body(me_ref, mb_ref, mt_ref, sel_ref, lab_ref, *, blocks):
    entries = me_ref.shape[1]
    devices = lab_ref.shape[0]
    shape = (devices, entries)
    owner = me_ref[...] >> 7
    place = (me_ref[...] & 127).astype(F32)
    lane = lax.broadcasted_iota(jnp.int32, shape, 0)
    owned = (lane == owner).astype(F32)
    before = lax.broadcasted_iota(jnp.int32, (entries, entries), 0) < lax.broadcasted_iota(
        jnp.int32, (entries, entries), 1
    )
    ahead = dot(owned.astype(BF16), before.astype(F32).astype(BF16))
    rank = jnp.sum(owned * ahead, axis=0, keepdims=True)
    combo = (lane == mt_ref[...] * blocks + mb_ref[...]).astype(F32).astype(BF16)
    for s in range(CAP):
        mine = jnp.where(rank == float(s), owned, 0.0).astype(BF16)
        pick = dot(mine, combo, ((1,), (1,))).astype(BF16)
        half = devices // 2
        for h in range(2):
            at = (h * CAP + s) * half
            for side in range(2):
                sel_ref[at : at + half, side * 128 : (side + 1) * 128] = pick[
                    h * half : (h + 1) * half
                ]
    spread = jnp.where(lane.astype(F32) == rank, place + 1.0, 0.0).astype(BF16)
    lab_ref[...] = dot(owned.astype(BF16), spread, ((1,), (1,)))


def pack_body(own_ref, part_ref, even_ref, odd_ref, tab_hbm, *refs, paired):
    if paired:
        margin_ref, out_hbm, sel_hbm, lab_hbm, sel_ref, lab_ref = refs[:6]
    else:
        sel_ref, lab_ref, out_hbm = refs[:3]
    src, mp, tab, out, sems = refs[-5:]
    planes, rows, width = own_ref.shape[1:]
    tables, nodes = tab.shape[0], tab.shape[1]
    blocks = 128 // tables
    loads = [pltpu.make_async_copy(tab_hbm.at[t], tab.at[t], sems.at[t]) for t in range(tables)]
    for load in loads:
        load.start()
    if paired:
        margin = [margin_ref.at[pl.ds(row, 1)] for row in range(3)]
        slots_body(*margin, sel_ref, lab_ref, blocks=blocks)
        kept = [
            pltpu.make_async_copy(sel_ref, sel_hbm, sems.at[tables + 2]),
            pltpu.make_async_copy(lab_ref, lab_hbm, sems.at[tables + 3]),
        ]
        for copy in kept:
            copy.start()
    low_flow = flags()[0] == 0

    def pick(when, other):
        return jnp.where(low_flow, when, other) if paired else when

    def turn(value, by):
        return pltpu.roll(value, by % width, 1)

    for x in range(planes):
        v = [own_ref[d, x] for d in range(3)]

        def along_x(d):
            if x == 0:
                below = pick(odd_ref[d, 0], even_ref[d, 0])
            else:
                below = own_ref[d, x - 1]
            if x == planes - 1:
                above = pick(even_ref[d, 0], odd_ref[d, 0])
            else:
                above = own_ref[d, x + 1]
            return 0.5 * (above - below)

        def along_y(d):
            both = jnp.concatenate([v[d], part_ref[d, x]], axis=0)
            up = pltpu.roll(both, 2 * rows - 1, 0)[:rows]
            down = pltpu.roll(both, 1, 0)[:rows]
            return 0.5 * (up - down)

        def along_z(d):
            return 0.5 * (turn(v[d], -1) - turn(v[d], 1))

        curl = (
            along_y(2) - along_z(1),
            along_z(0) - along_x(2),
            along_x(1) - along_y(0),
        )
        for c in range(3):
            a, b = (c + 1) % 3, (c + 2) % 3
            base = (c * planes + x) * rows
            lamb = curl[a] * v[b] - curl[b] * v[a]
            src[0, base : base + rows, :] = lamb[:, :128]
            src[1, base : base + rows, :] = lamb[:, 128:]
    count = 3 * blocks
    split = [
        halves(src[half, pl.ds(start, count, stride=2), :])
        for start in range(2)
        for half in range(2)
    ]
    left = jnp.concatenate(
        [
            jnp.concatenate([h for h, _ in split], axis=1),
            jnp.concatenate([l for _, l in split], axis=1),
        ],
        axis=0,
    )
    for t in range(tables):
        loads[t].wait()
        high, low = halves(tab[t])
        wide = dot(left, high)
        mapped = wide[:count] + wide[count:] + dot(left[:count], low)
        for c in range(3):
            high, low = halves(mapped[c * blocks : (c + 1) * blocks])
            mp[c, t * blocks : (t + 1) * blocks, :] = high
            mp[c, 128 + t * blocks : 128 + (t + 1) * blocks, :] = low
    devices = sel_ref.shape[0] // CAP
    half = devices // 2
    groups = nodes // 128
    stride = out.shape[0] // devices
    out[pl.ds(stride - 1, devices, stride=stride), :] = lab_ref[...]
    stores = []
    for h in range(2):
        for c in range(3):
            filled = dot(sel_ref[h * CAP * half : (h + 1) * CAP * half, :], mp[c])
            for s in range(CAP):
                for m in range(groups):
                    row = h * half * stride + CAP * (c * groups + m) + s
                    out[pl.ds(row, half, stride=stride), :] = filled[
                        s * half : (s + 1) * half, m * 128 : (m + 1) * 128
                    ]
        part = pl.ds(h * half * stride, half * stride)
        store = pltpu.make_async_copy(out.at[part], out_hbm.at[part], sems.at[tables + h])
        store.start()
        stores.append(store)
    for store in stores + (kept if paired else []):
        store.wait()


def primitives(s):
    inverse = 1.0 / s[0]
    v = [s[1 + d] * inverse for d in range(3)]
    kinetic = v[0] * v[0] + v[1] * v[1] + v[2] * v[2]
    p = (GAMMA - 1.0) * (s[4] - 0.5 * s[0] * kinetic)
    return v, p, jnp.sqrt(GAMMA * p * inverse)


def flux_of(s, v, p, d, k):
    if k == 0:
        return s[1 + d]
    if k == 4:
        return (s[4] + p) * v
    product = s[k] * v
    return product + p if k == 1 + d else product


def flow_stage(src, base, dst, prim, first, last, weights, shift=0, rows=None):
    a_weight, b_weight = weights

    def prepare(x, carry):
        v, p, sound = primitives([src[k, x] for k in range(5)])
        for d in range(3):
            prim[d, x] = v[d]
        prim[3, x] = p
        prim[4, x] = sound
        return carry

    lax.fori_loop(first - 1, last + 1, prepare, 0)

    def advance(x, carry):
        s = [src[k, x] for k in range(5)]
        total = []
        sound = prim[4, x]
        p = prim[3, x]
        up = [src[k, x + 1] for k in range(5)]
        down = [src[k, x - 1] for k in range(5)]
        v, vu, vd = prim[0, x], prim[0, x + 1], prim[0, x - 1]
        speed = jnp.abs(v) + sound
        fast_u = jnp.maximum(speed, jnp.abs(vu) + prim[4, x + 1])
        fast_d = jnp.maximum(speed, jnp.abs(vd) + prim[4, x - 1])
        pu, pd = prim[3, x + 1], prim[3, x - 1]
        for k in range(5):
            jump = fast_u * (up[k] - s[k]) - fast_d * (s[k] - down[k])
            total.append(flux_of(up, vu, pu, 0, k) - flux_of(down, vd, pd, 0, k) - jump)
        for d, axis in ((1, 0), (2, 1)):
            size = s[0].shape[axis]
            v = prim[d, x]
            speed = jnp.abs(v) + sound
            fast = jnp.maximum(speed, pltpu.roll(speed, size - 1, axis))
            for k in range(5):
                flux = flux_of(s, v, p, d, k)
                face = flux + pltpu.roll(flux, size - 1, axis)
                face = face - fast * (pltpu.roll(s[k], size - 1, axis) - s[k])
                total[k] = total[k] + (face - pltpu.roll(face, 1, axis))
        for k in range(5):
            value = b_weight * s[k] - (0.5 * DT_FLOW * b_weight) * total[k]
            if a_weight is not None:
                value = value + a_weight * base[k, x]
            if rows is not None:
                value = value[:rows]
            dst[k, x - shift] = value
        return carry

    lax.fori_loop(first, last, advance, 0)


STAGES = ((None, 1.0), (0.75, 0.25), (1.0 / 3.0, 2.0 / 3.0))


def place(s0, start, mine, other, first=0):
    rows = mine.shape[2]
    for i in range(mine.shape[1]):
        for k in range(5):
            s0[k, start + first + i, :rows] = mine[k, i]
            s0[k, start + first + i, rows:] = other[k, i]


def around_own(planes):
    above = jnp.where(flags()[0] == 0, 2 * planes, 0)
    return above, 2 * planes - above


def first_flow_body(*refs):
    mine, other = refs[:3], refs[3:6]
    new_own, new_part, mid, low, high = refs[6:11]
    own_ref, part_ref, lo_ref, hi_ref = refs[11:15]
    s0, s1, s2, prim = refs[15:]
    planes, rows = mine[0].shape[1], mine[0].shape[2]
    for start, a, b in zip((planes, *around_own(planes)), mine, other):
        place(s0, start, a, b)
    wide = 3 * planes
    flow_stage(s0, None, s1, prim, 1, wide - 1, STAGES[0])
    flow_stage(s1, s0, s2, prim, 2, wide - 2, STAGES[1])
    flow_stage(s2, s0, s1, prim, 3, wide - 3, STAGES[2])
    for i in range(-1, planes + 1):
        x = planes + i
        inverse = 1.0 / s1[0, x]
        v = [s1[1 + d, x] * inverse for d in range(3)]
        for d in range(3):
            if i == -1:
                lo_ref[d, 0] = v[d][:rows]
            elif i == planes:
                hi_ref[d, 0] = v[d][:rows]
            else:
                own_ref[d, i] = v[d][:rows]
                part_ref[d, i] = v[d][rows:]
        for k in range(5):
            if i == -1:
                low[k, 0] = s1[k, x]
            elif i == planes:
                high[k, 0] = s1[k, x]
            else:
                new_own[k, i] = s1[k, x, :rows]
                new_part[k, i] = s1[k, x, rows:]
                if 0 < i < planes - 1:
                    mid[k, i - 1] = s1[k, x, :rows]


def last_flow_body(*refs):
    own, part, low, high = refs[:4]
    even, odd, even_part, odd_part, out_ref = refs[4:9]
    s0, s1, s2, prim = refs[9:]
    planes, rows = own.shape[1], own.shape[2]
    place(s0, planes, own, part)
    even_at, odd_at = around_own(planes)
    place(s0, even_at, even, even_part, first=1)
    place(s0, odd_at, odd, odd_part, first=1)
    wide = 3 * planes
    for k in range(5):
        s0[k, planes - 1] = low[k, 0]
        s0[k, 2 * planes] = high[k, 0]
    flow_stage(s0, None, s1, prim, 2, wide - 2, STAGES[0])
    flow_stage(s1, s0, s2, prim, 3, wide - 3, STAGES[1])
    flow_stage(s2, s0, out_ref, prim, planes, 2 * planes, STAGES[2], shift=planes, rows=rows)


def derive(values):
    half = NP // 2
    even = [values[i] + values[NP - 1 - i] for i in range(half)]
    odd = [values[i] - values[NP - 1 - i] for i in range(half)]
    tops, bottoms = [], []
    for a in range(half):
        plus = minus = None
        for i in range(half):
            ce = 0.5 * float(MATRIX[a, i] + MATRIX[a, NP - 1 - i])
            co = 0.5 * float(MATRIX[a, i] - MATRIX[a, NP - 1 - i])
            te, to = ce * even[i], co * odd[i]
            plus = te if plus is None else plus + te
            minus = to if minus is None else minus + to
        tops.append(plus + minus)
        bottoms.append(minus - plus)
    return tops + bottoms[::-1]


def along_middle(ps, us, lanes):
    p = derive(ps)
    below, above = (ps[-1], -ps[0]) if us is None else (ps[-1] + us[-1], us[0] - ps[0])
    own_low, own_high = (ps[0], -ps[-1]) if us is None else (ps[0] + us[0], us[-1] - ps[-1])
    low = LIFT * (pltpu.roll(below, EZ, 1) - own_low)
    high = LIFT * (pltpu.roll(above, lanes - EZ, 1) - own_high)
    dp = [None] * NP if us is None else [-u for u in derive(us)]
    du = [-value for value in p]
    dp[0] = low if dp[0] is None else dp[0] + low
    dp[-1] = -high if dp[-1] is None else dp[-1] - high
    du[0] = du[0] + low
    du[-1] = du[-1] + high
    return dp, du


def inner_maker(coef, lanes):
    lane = lax.broadcasted_iota(jnp.int32, (NP, lanes), 1)
    row = lax.broadcasted_iota(jnp.int32, (NP, lanes), 0)
    firsts = (lane & (EZ - 1)) == 0
    lasts = (lane & (EZ - 1)) == EZ - 1
    is_low = row == 0
    lift_u = jnp.where(is_low | (row == NP - 1), LIFT, 0.0)
    lift_p = jnp.where(is_low, LIFT, jnp.where(row == NP - 1, -LIFT, 0.0))

    def slope(value):
        total = coef[0] * value
        for k in range(1, NP):
            total = total + coef[k] * pltpu.roll(value, NP - k, 0)
        return total

    def jump_of(p, u):
        up, down = (p, -p) if u is None else (u + p, u - p)
        edge = jnp.where(is_low, pltpu.roll(up, 1, 0), pltpu.roll(down, NP - 1, 0))
        from_low = jnp.where(firsts, pltpu.roll(edge, lanes + 1 - EZ, 1), pltpu.roll(edge, 1, 1))
        from_high = jnp.where(
            lasts, pltpu.roll(edge, EZ - 1, 1), pltpu.roll(edge, lanes - 1, 1)
        )
        return jnp.where(is_low, from_low - up, from_high - down)

    def both(p, u, want_u=True):
        jump = jump_of(p, u)
        dp = lift_p * jump if u is None else lift_p * jump - slope(u)
        return dp, (lift_u * jump - slope(p)) if want_u else None

    return both


def local_rate(s, r, coef, forcing=None):
    lanes = s.shape[-1]

    def first(j, carry):
        p = derive([s[0, i, j] for i in range(NP)])
        u = derive([s[1, i, j] for i in range(NP)])
        for i in range(NP):
            r[0, i, j] = -u[i]
            r[1, i, j] = -p[i] if forcing is None else forcing[0, i, j] - p[i]
        return carry

    lax.fori_loop(0, NP, first, 0)
    inner = inner_maker(coef, lanes)

    def second(i, carry):
        ps = [s[0, i, j] for j in range(NP)]
        dp, du = along_middle(ps, [s[2, i, j] for j in range(NP)], lanes)
        for j in range(NP):
            dq, dw = inner(ps[j], s[3, i, j])
            r[0, i, j] = r[0, i, j] + (dp[j] + dq)
            r[2, i, j] = du[j] if forcing is None else forcing[1, i, j] + du[j]
            r[3, i, j] = dw if forcing is None else forcing[2, i, j] + dw
        return carry

    lax.fori_loop(0, NP, second, 0)


def each(function):
    def body(i, carry):
        function(i)
        return carry

    lax.fori_loop(0, NP, body, 0)


LAST = NP - 1


def chosen(low, when_low, when_high):
    return jnp.where(low, when_low, when_high)


def add_lifts(s, r, incoming=None):
    def lift(j):
        from_low, from_high = (0.0, 0.0) if incoming is None else incoming(j)
        low = LIFT * (from_low - (s[1, 0, j] + s[0, 0, j]))
        high = LIFT * (from_high - (s[1, LAST, j] - s[0, LAST, j]))
        r[0, 0, j] = r[0, 0, j] + low
        r[1, 0, j] = r[1, 0, j] + low
        r[0, LAST, j] = r[0, LAST, j] - high
        r[1, LAST, j] = r[1, LAST, j] + high

    each(lift)


def ends_body(w, even, odd):
    low_core = flags()[1] == 0
    up, down = w[0, LAST] + w[1, LAST], w[1, 0] - w[0, 0]
    even[...] = chosen(low_core, up, down)
    odd[...] = chosen(low_core, down, up)


def rate_body(w, even, odd, coef, r):
    low_core = flags()[1] == 0
    local_rate(w, r, coef)
    add_lifts(
        w,
        r,
        lambda j: (
            chosen(low_core, odd[j], even[j]),
            chosen(low_core, even[j], odd[j]),
        ),
    )


def unpack_body(w, r0, arrived_hbm, coef, f, s1, even, odd, arrived, wide, sums, sems):
    lanes = w.shape[-1]
    groups = sums.shape[0]
    stride = groups * CAP + 1
    half = arrived.shape[0] // stride // 2
    loads = []
    for h in range(2):
        part = pl.ds(h * half * stride, half * stride)
        loads.append(pltpu.make_async_copy(arrived_hbm.at[part], arrived.at[part], sems.at[h]))
        loads[-1].start()
    row = lax.broadcasted_iota(jnp.int32, (lanes, half), 0).astype(F32)
    for h in range(2):
        loads[h].wait()
        base = h * half * stride
        labels = arrived[pl.ds(base + stride - 1, half, stride=stride), :].T
        pick = jnp.concatenate(
            [(row == labels[s : s + 1] - 1.0).astype(F32).astype(BF16) for s in range(CAP)],
            axis=1,
        )
        for g in range(groups):
            for s in range(CAP):
                part = arrived[pl.ds(base + CAP * g + s, half, stride=stride), :]
                high, low = halves(part)
                wide[g % 2, s * half : (s + 1) * half, 0:128] = high
                wide[g % 2, s * half : (s + 1) * half, 128:256] = low
            both = dot(pick, wide[g % 2])
            if h == 0:
                sums[g] = both
                continue
            both = both + sums[g]
            nodes = (both[:, :128] + both[:, 128:]).T
            for row_of in range(128 // NP):
                at = g * 128 // NP + row_of
                c, i, j = at // (NP * NP), at // NP % NP, at % NP
                f[c, i, j] = nodes[row_of * NP : (row_of + 1) * NP, :]

    def add(i):
        for k in range(4):
            rate = r0[k, i] if k == 0 else r0[k, i] + f[k - 1, i]
            s1[k, i] = w[k, i] + DT_WAVE * rate

    each(add)
    inner = inner_maker(coef, lanes)
    low_core = flags()[1] == 0
    now, then = [], []
    for i, sign in ((LAST, 1.0), (0, -1.0)):
        ps = [s1[0, i, j] for j in range(NP)]
        dp, _ = along_middle(ps, [s1[2, i, j] for j in range(NP)], lanes)
        now_rows, then_rows = [], []
        for j in range(NP):
            dq, _ = inner(ps[j], s1[3, i, j], want_u=False)
            rate_p = dp[j] + dq
            rate_u = f[0, i, j]
            for m in range(NP):
                c = float(MATRIX[i, m])
                if c != 0.0:
                    rate_p = rate_p - c * s1[1, m, j]
                    rate_u = rate_u - c * s1[0, m, j]
            u = s1[1, i, j]
            next_p = 0.75 * w[0, i, j] + 0.25 * (ps[j] + DT_WAVE * rate_p)
            next_u = 0.75 * w[1, i, j] + 0.25 * (u + DT_WAVE * rate_u)
            now_rows.append(u + sign * ps[j])
            then_rows.append(next_u + sign * next_p)
        now.append(now_rows)
        then.append(then_rows)
    for j in range(NP):
        for slot, (up, down) in enumerate((now, then)):
            even[slot, j] = chosen(low_core, up[j], down[j])
            odd[slot, j] = chosen(low_core, down[j], up[j])


def middle_body(w, s1, f, coef, s2, r2, r1):
    local_rate(s1, r1, coef, f)
    add_lifts(s1, r1)

    def add(i):
        for k in range(4):
            s2[k, i] = 0.75 * w[k, i] + 0.25 * (s1[k, i] + DT_WAVE * r1[k, i])

    each(add)
    local_rate(s2, r2, coef, f)
    add_lifts(s2, r2)


def relay_body(w, s1, f, coef, even, odd, s2, r2, even3, odd3, far_even, far_odd, r1):
    middle_body(w, s1, f, coef, s2, r2, r1)
    low_flow, low_core = flags()[0] == 0, flags()[1] == 0

    def third(k, i, j):
        return w[k, i, j] * (1.0 / 3.0) + (2.0 / 3.0) * (s2[k, i, j] + DT_WAVE * r2[k, i, j])

    def send(j):
        for slot in range(2):
            even3[slot, j] = even[slot, j]
            odd3[slot, j] = odd[slot, j]
        up = third(1, LAST, j) + third(0, LAST, j)
        down = third(1, 0, j) - third(0, 0, j)
        even3[2, j] = chosen(low_core, up, down)
        odd3[2, j] = chosen(low_core, down, up)
        up = chosen(low_core, even[0, j], odd[0, j])
        down = chosen(low_core, odd[0, j], even[0, j])
        far_even[j] = chosen(low_flow, up, down)
        far_odd[j] = chosen(low_flow, down, up)

    each(send)


def close_step(w, s2, r2, even, odd, coef, out, s, r):
    lanes = w.shape[-1]
    low_core = flags()[1] == 0

    def first(j):
        low = (0.25 * DT_WAVE * LIFT) * chosen(low_core, odd[0, j], even[0, j])
        high = (0.25 * DT_WAVE * LIFT) * chosen(low_core, even[0, j], odd[0, j])
        s[0, j] = low
        s[1, j] = -high
        lift_low = LIFT * (chosen(low_core, odd[1, j], even[1, j]) - 2.0 * low)
        lift_high = LIFT * (chosen(low_core, even[1, j], odd[1, j]) - 2.0 * high)
        for i in range(NP):
            a, b = float(MATRIX[i, 0]), float(MATRIX[i, LAST])
            p = r2[0, i, j] - a * low - b * high
            u = r2[1, i, j] - a * low + b * high
            if i == 0:
                p, u = p + lift_low, u + lift_low
            if i == LAST:
                p, u = p - lift_high, u + lift_high
            r[0, i, j] = p
            r[1, i, j] = u

    each(first)
    third = 1.0 / 3.0

    def close(k, i, j, state, rate):
        out[k, i, j] = w[k, i, j] * third + (2.0 * third) * (state + DT_WAVE * rate)

    def inside(i, carry):
        for j in range(NP):
            for k in range(4):
                rate = r[k, i, j] if k < 2 else r2[k, i, j]
                close(k, i, j, s2[k, i, j], rate)
        return carry

    lax.fori_loop(1, LAST, inside, 0)
    inner = inner_maker(coef, lanes)
    for side, i in ((0, 0), (1, LAST)):
        ps = [s[side, j] for j in range(NP)]
        dp, du = along_middle(ps, None, lanes)
        for j in range(NP):
            dq, dw = inner(ps[j], None)
            rate = r[0, i, j] + dq
            if dp[j] is not None:
                rate = rate + dp[j]
            close(0, i, j, s2[0, i, j] + ps[j], rate)
            change = ps[j] if side == 0 else -ps[j]
            close(1, i, j, s2[1, i, j] + change, r[1, i, j])
            close(2, i, j, s2[2, i, j], r2[2, i, j] + du[j])
            close(3, i, j, s2[3, i, j], r2[3, i, j] + dw)


def turn_body(
    w, s2, r2, even, odd, far_even, far_odd, own_even, own_odd, coef, out, r0, s, r, q
):
    close_step(w, s2, r2, even, odd, coef, out, s, r)
    lanes = w.shape[-1]
    low_flow, low_core = flags()[0] == 0, flags()[1] == 0
    inner = inner_maker(coef, lanes)
    weight = 0.25 * DT_WAVE * LIFT

    def spill(values):
        dp, _ = along_middle(values, None, lanes)
        found = []
        for j in range(NP):
            dq, _ = inner(values[j], None, want_u=False)
            found.append(dq if dp[j] is None else dp[j] + dq)
        return found

    ups = [weight * chosen(low_core, own_even[0, j], own_odd[0, j]) for j in range(NP)]
    downs = [weight * chosen(low_core, own_odd[0, j], own_even[0, j]) for j in range(NP)]
    step = 2.0 / 3.0 * DT_WAVE
    for j, (a, b) in enumerate(zip(spill([-d for d in downs]), spill(ups))):
        far_low = chosen(low_flow, far_odd[j], far_even[j])
        far_high = chosen(low_flow, far_even[j], far_odd[j])
        a = a - (2.0 * float(MATRIX[LAST, 0]) * weight) * far_low
        b = (2.0 * float(MATRIX[0, LAST]) * weight) * far_high - b
        q[0, j] = chosen(low_core, odd[2, j], even[2, j]) + step * a
        q[1, j] = chosen(low_core, even[2, j], odd[2, j]) + step * b
    local_rate(out, r0, coef)
    add_lifts(out, r0, lambda j: (q[0, j], q[1, j]))


def trade(value, axis, odd):
    size = lax.axis_size(axis)
    pairs = []
    for i in range(odd, size + odd, 2):
        a, b = i % size, (i + 1) % size
        pairs += [(a, b), (b, a)]
    return lax.ppermute(value, axis, pairs)


def exchange_all(value):
    return lax.all_to_all(value, AXES, split_axis=0, concat_axis=0, tiled=True)


def advance(density, velocity, pressure, wave, tables, margin_element, margin_block, margin_table):
    planes, rows, width = density.shape
    lanes = wave.shape[-1]
    devices = lax.axis_size("flow") * lax.axis_size("group")
    kinds, nodes = tables.shape[:2]

    coef = np.stack([MATRIX[np.arange(NP), (np.arange(NP) + k) % NP] for k in range(NP)])
    coef = jnp.asarray(np.broadcast_to(coef[:, :, None], (NP, NP, lanes)).copy())
    odd_flow = lax.axis_index("flow") & 1

    inward = (planes - 1) * (1 - odd_flow)
    v_even = trade(lax.dynamic_slice_in_dim(velocity, inward, 1, 1), "flow", 0)
    v_odd = trade(lax.dynamic_slice_in_dim(velocity, planes - 1 - inward, 1, 1), "flow", 1)
    v_part = trade(velocity, "group", 0)

    block = sds(5, planes, rows, width)
    fields, margin = call(
        fields_body,
        (block, sds(8, margin_element.shape[1], dtype=jnp.int32)),
        1_000_000,
        limit=WHOLE_VMEM,
    )(density, velocity, pressure, margin_element, margin_block, margin_table)

    def surround(own):
        even = trade(own, "flow", 0)
        return (own, even, trade(own, "flow", 1))

    def swap_rows(pieces):
        return [trade(p, "group", 0) for p in pieces]

    pieces = surround(fields)
    others = swap_rows(pieces)

    def send(speeds, extra, length, out_shape=(), **keys):
        sent = sds(devices * length, 128)
        sent = call(
            lambda *refs: pack_body(*refs, paired=bool(out_shape)),
            (sent, *out_shape) if out_shape else sent,
            8_000_000,
            scratch=(
                *(pltpu.VMEM(o.shape, o.dtype) for o in out_shape),
                pltpu.VMEM((2, 3 * planes * rows, 128), F32),
                pltpu.VMEM((3, 256, nodes), BF16),
                pltpu.VMEM(tables.shape, F32),
                pltpu.VMEM((devices * length, 128), F32),
                pltpu.SemaphoreType.DMA((kinds + 4,)),
            ),
            limit=PACK_VMEM,
            **keys,
        )(*speeds, tables, *extra)
        sent, *kept = sent if out_shape else (sent,)
        sent = exchange_all(sent.reshape(devices, 1, length * 128))
        return sent.reshape(devices * length, 128), kept

    stride = 3 * CAP * nodes // 128 + 1
    arrived_1, kept = send(
        (velocity, v_part, v_even, v_odd),
        (margin,),
        stride,
        (sds(CAP * devices, 256, dtype=BF16), sds(devices, 128)),
        specs="vvvvhv",
        out_specs="hhh",
    )

    speed = sds(3, planes, rows, width)
    thin = sds(3, 1, rows, width)
    edge = sds(5, 1, 2 * rows, width)
    wide = pltpu.VMEM((5, 3 * planes, 2 * rows, width), F32)
    new_own, new_part, mid, low_edge, high_edge, own, part, low, high = call(
        first_flow_body,
        (block, block, sds(5, planes - 2, rows, width), edge, edge, speed, speed, thin, thin),
        60_000_000,
        scratch=[wide] * 4,
    )(*pieces, *others)
    arrived_2, _ = send((own, part, high, low), kept, stride, specs="vvvvhvv", out_specs="h")
    mids = surround(mid)[1:]

    def finish_flow(mids):
        return call(last_flow_body, block, 30_000_000, scratch=[wide] * 4)(
            new_own, new_part, low_edge, high_edge, *mids, *swap_rows(mids)
        )

    state = sds(*wave.shape)
    force = sds(3, *wave.shape[1:])
    hold = pltpu.VMEM(wave.shape, F32)
    face = sds(NP, NP, lanes)
    pair = sds(2, NP, NP, lanes)
    triple = sds(3, NP, NP, lanes)
    sides = pltpu.VMEM((2, NP, NP, lanes), F32)
    couple = pltpu.VMEM((2,) + wave.shape[1:], F32)
    unpack = call(
        unpack_body,
        (force, state, pair, pair),
        12_000_000,
        scratch=[
            pltpu.VMEM((devices * stride, 128), F32),
            pltpu.VMEM((2, CAP * devices // 2, 256), BF16),
            pltpu.VMEM((3 * nodes // 128, lanes, 256), F32),
            pltpu.SemaphoreType.DMA((2,)),
        ],
        specs="vvhv",
    )

    def around(even, odd):
        return (trade(even, "group", 0), trade(odd, AXES, 1))

    ends = call(ends_body, (face, face), 100_000)(wave)
    faces = around(*ends)
    rate = call(rate_body, state, 8_000_000)(wave, *faces, coef)
    forcing, s1, *ends = unpack(wave, rate, arrived_1, coef)
    s2, r2, even, odd, far_even, far_odd = call(
        relay_body, (state, state, triple, triple, face, face), 16_000_000, scratch=[hold]
    )(wave, s1, forcing, coef, *ends)
    faces = around(even, odd)
    far = (trade(far_even, "flow", 0), trade(far_odd, "flow", 1))
    mids, _ = lax.optimization_barrier((mids, far_even))
    flow_state = finish_flow(mids)
    wave, rate = call(
        turn_body, (state, state), 14_000_000, scratch=[sides, couple, sides]
    )(wave, s2, r2, *faces, *far, *ends, coef)

    forcing, s1, *ends = unpack(wave, rate, arrived_2, coef)
    faces = around(*ends)
    s2, r2 = call(middle_body, (state, state), 16_000_000, scratch=[hold])(wave, s1, forcing, coef)
    wave = call(close_step, state, 6_000_000, scratch=[sides, couple])(wave, s2, r2, *faces, coef)
    return (flow_state, wave, forcing)


def solution(mesh):
    in_specs = (
        P("flow", "group", None),
        P(None, "flow", "group", None),
        P("flow", "group", None),
        P(None, None, None, None, AXES),
        P(),
        P(AXES, None),
        P(AXES, None),
        P(AXES, None),
    )
    out_specs = (
        P(None, "flow", "group", None),
        P(None, None, None, None, AXES),
        P(None, None, None, None, AXES),
    )
    return jax.shard_map(advance, mesh=mesh, in_specs=in_specs, out_specs=out_specs, check_vma=False)
```

```python
import jax
import jax.numpy as jnp
import numpy as np
from jax import lax
from jax.experimental import pallas as pl
from jax.experimental.pallas import tpu as pltpu
from jax.sharding import PartitionSpec as P


NP = 8
EZ = 16
CAP = 4
GAMMA = 1.4
DT_FLOW = 0.08
DT_WAVE = 0.01
F32 = jnp.float32
BF16 = jnp.bfloat16
AXES = ("flow", "group")
VMEM_LIMIT = 26 * 2**20
WHOLE_VMEM = 63_050_000
PACK_VMEM = 55_000_000


def legendre_pair(nodes, degree):
    previous = np.ones(nodes.shape[0])
    current = nodes * 1.0
    for order in range(2, degree + 1):
        previous, current = (
            current,
            ((2 * order - 1) * nodes * current - (order - 1) * previous) / order,
        )
    return (previous, current)


def lobatto(point_count):
    degree = point_count - 1
    nodes = -np.cos(np.pi * np.arange(point_count) / degree)
    for _ in range(60):
        previous, current = legendre_pair(nodes, degree)
        nodes = nodes - (nodes * current - previous) / (point_count * current)
    previous, values = legendre_pair(nodes, degree)
    weights = 2.0 / (degree * (degree + 1) * values**2)
    identity = np.eye(point_count)
    differ = nodes[:, None] - nodes[None, :] + identity
    matrix = values[:, None] / values[None, :] / differ * (1.0 - identity)
    matrix[0, 0] = -degree * (degree + 1) / 4.0
    matrix[-1, -1] = degree * (degree + 1) / 4.0
    return (matrix.astype(np.float32), float(weights[0]))


MATRIX, END_WEIGHT = lobatto(NP)
LIFT = 0.5 / END_WEIGHT


def sds(*shape, dtype=F32):
    return jax.ShapeDtypeStruct(shape, dtype)


def call(body, out_shape, flops, scratch=(), specs=None, out_specs=None, limit=VMEM_LIMIT):
    kinds = {"s": pltpu.SMEM, "v": pltpu.VMEM, "h": pltpu.HBM}
    extra = {}
    if specs is not None:
        extra["in_specs"] = [pl.BlockSpec(memory_space=kinds[k]) for k in specs]
    if out_specs is not None:
        places = [pl.BlockSpec(memory_space=kinds[k]) for k in out_specs]
        extra["out_specs"] = places if len(places) > 1 else places[0]
    return pl.pallas_call(
        body,
        out_shape=out_shape,
        scratch_shapes=list(scratch),
        cost_estimate=pl.CostEstimate(flops=flops, bytes_accessed=4_000_000, transcendentals=0),
        compiler_params=pltpu.CompilerParams(vmem_limit_bytes=limit),
        **extra,
    )


def flags():
    return lax.axis_index("flow") & 1, lax.axis_index("group")


def halves(value):
    high = value.astype(BF16)
    return high, (value - high.astype(F32)).astype(BF16)


def dot(left, right, dims=((1,), (0,))):
    return lax.dot_general(left, right, (dims, ((), ())), preferred_element_type=F32)


def fields_body(rho_ref, vel_ref, pre_ref, me_ref, mb_ref, mt_ref, f_ref, margin_ref):
    for row, ref in enumerate((me_ref, mb_ref, mt_ref)):
        margin_ref[row : row + 1, :] = ref[...]
    rho = rho_ref[...]
    v = [vel_ref[d] for d in range(3)]
    kinetic = v[0] * v[0] + v[1] * v[1] + v[2] * v[2]
    f_ref[0] = rho
    for d in range(3):
        f_ref[1 + d] = rho * v[d]
    f_ref[4] = pre_ref[...] / (GAMMA - 1.0) + 0.5 * rho * kinetic


def slots_body(me_ref, mb_ref, mt_ref, sel_ref, lab_ref, *, blocks):
    entries = me_ref.shape[1]
    devices = lab_ref.shape[0]
    shape = (devices, entries)
    owner = me_ref[...] >> 7
    place = (me_ref[...] & 127).astype(F32)
    lane = lax.broadcasted_iota(jnp.int32, shape, 0)
    owned = (lane == owner).astype(F32)
    before = lax.broadcasted_iota(jnp.int32, (entries, entries), 0) < lax.broadcasted_iota(
        jnp.int32, (entries, entries), 1
    )
    ahead = dot(owned.astype(BF16), before.astype(F32).astype(BF16))
    rank = jnp.sum(owned * ahead, axis=0, keepdims=True)
    combo = (lane == mt_ref[...] * blocks + mb_ref[...]).astype(F32).astype(BF16)
    for s in range(CAP):
        mine = jnp.where(rank == float(s), owned, 0.0).astype(BF16)
        pick = dot(mine, combo, ((1,), (1,))).astype(BF16)
        half = devices // 2
        for h in range(2):
            at = (h * CAP + s) * half
            for side in range(2):
                sel_ref[at : at + half, side * 128 : (side + 1) * 128] = pick[
                    h * half : (h + 1) * half
                ]
    spread = jnp.where(lane.astype(F32) == rank, place + 1.0, 0.0).astype(BF16)
    lab_ref[...] = dot(owned.astype(BF16), spread, ((1,), (1,)))


def pack_body(own_ref, part_ref, even_ref, odd_ref, tab_hbm, *refs, paired):
    if paired:
        margin_ref, out_hbm, sel_hbm, lab_hbm, sel_ref, lab_ref = refs[:6]
    else:
        sel_ref, lab_ref, out_hbm = refs[:3]
    src, mp, tab, out, sems = refs[-5:]
    planes, rows, width = own_ref.shape[1:]
    tables, nodes = tab.shape[0], tab.shape[1]
    blocks = 128 // tables
    loads = [pltpu.make_async_copy(tab_hbm.at[t], tab.at[t], sems.at[t]) for t in range(tables)]
    for load in loads:
        load.start()
    if paired:
        margin = [margin_ref.at[pl.ds(row, 1)] for row in range(3)]
        slots_body(*margin, sel_ref, lab_ref, blocks=blocks)
        kept = [
            pltpu.make_async_copy(sel_ref, sel_hbm, sems.at[tables + 2]),
            pltpu.make_async_copy(lab_ref, lab_hbm, sems.at[tables + 3]),
        ]
        for copy in kept:
            copy.start()
    low_flow = flags()[0] == 0

    def pick(when, other):
        return jnp.where(low_flow, when, other) if paired else when

    def turn(value, by):
        return pltpu.roll(value, by % width, 1)

    for x in range(planes):
        v = [own_ref[d, x] for d in range(3)]

        def along_x(d):
            if x == 0:
                below = pick(odd_ref[d, 0], even_ref[d, 0])
            else:
                below = own_ref[d, x - 1]
            if x == planes - 1:
                above = pick(even_ref[d, 0], odd_ref[d, 0])
            else:
                above = own_ref[d, x + 1]
            return 0.5 * (above - below)

        def along_y(d):
            both = jnp.concatenate([v[d], part_ref[d, x]], axis=0)
            up = pltpu.roll(both, 2 * rows - 1, 0)[:rows]
            down = pltpu.roll(both, 1, 0)[:rows]
            return 0.5 * (up - down)

        def along_z(d):
            return 0.5 * (turn(v[d], -1) - turn(v[d], 1))

        curl = (
            along_y(2) - along_z(1),
            along_z(0) - along_x(2),
            along_x(1) - along_y(0),
        )
        for c in range(3):
            a, b = (c + 1) % 3, (c + 2) % 3
            base = (c * planes + x) * rows
            lamb = curl[a] * v[b] - curl[b] * v[a]
            src[0, base : base + rows, :] = lamb[:, :128]
            src[1, base : base + rows, :] = lamb[:, 128:]
    count = 3 * blocks
    split = [
        halves(src[half, pl.ds(start, count, stride=2), :])
        for start in range(2)
        for half in range(2)
    ]
    left = jnp.concatenate(
        [
            jnp.concatenate([h for h, _ in split], axis=1),
            jnp.concatenate([l for _, l in split], axis=1),
        ],
        axis=0,
    )
    for t in range(tables):
        loads[t].wait()
        high, low = halves(tab[t])
        wide = dot(left, high)
        mapped = wide[:count] + wide[count:] + dot(left[:count], low)
        for c in range(3):
            high, low = halves(mapped[c * blocks : (c + 1) * blocks])
            mp[c, t * blocks : (t + 1) * blocks, :] = high
            mp[c, 128 + t * blocks : 128 + (t + 1) * blocks, :] = low
    devices = sel_ref.shape[0] // CAP
    half = devices // 2
    groups = nodes // 128
    stride = out.shape[0] // devices
    out[pl.ds(stride - 1, devices, stride=stride), :] = lab_ref[...]
    stores = []
    for h in range(2):
        for c in range(3):
            filled = dot(sel_ref[h * CAP * half : (h + 1) * CAP * half, :], mp[c])
            for s in range(CAP):
                for m in range(groups):
                    row = h * half * stride + CAP * (c * groups + m) + s
                    out[pl.ds(row, half, stride=stride), :] = filled[
                        s * half : (s + 1) * half, m * 128 : (m + 1) * 128
                    ]
        part = pl.ds(h * half * stride, half * stride)
        store = pltpu.make_async_copy(out.at[part], out_hbm.at[part], sems.at[tables + h])
        store.start()
        stores.append(store)
    for store in stores + (kept if paired else []):
        store.wait()


def primitives(s):
    inverse = 1.0 / s[0]
    v = [s[1 + d] * inverse for d in range(3)]
    kinetic = v[0] * v[0] + v[1] * v[1] + v[2] * v[2]
    p = (GAMMA - 1.0) * (s[4] - 0.5 * s[0] * kinetic)
    return v, p, jnp.sqrt(GAMMA * p * inverse)


def flux_of(s, v, p, d, k):
    if k == 0:
        return s[1 + d]
    if k == 4:
        return (s[4] + p) * v
    product = s[k] * v
    return product + p if k == 1 + d else product


def flow_stage(src, base, dst, prim, first, last, weights, shift=0, rows=None):
    a_weight, b_weight = weights

    def prepare(x, carry):
        v, p, sound = primitives([src[k, x] for k in range(5)])
        for d in range(3):
            prim[d, x] = v[d]
        prim[3, x] = p
        prim[4, x] = sound
        return carry

    lax.fori_loop(first - 1, last + 1, prepare, 0)

    def advance(x, carry):
        s = [src[k, x] for k in range(5)]
        total = []
        sound = prim[4, x]
        p = prim[3, x]
        up = [src[k, x + 1] for k in range(5)]
        down = [src[k, x - 1] for k in range(5)]
        v, vu, vd = prim[0, x], prim[0, x + 1], prim[0, x - 1]
        speed = jnp.abs(v) + sound
        fast_u = jnp.maximum(speed, jnp.abs(vu) + prim[4, x + 1])
        fast_d = jnp.maximum(speed, jnp.abs(vd) + prim[4, x - 1])
        pu, pd = prim[3, x + 1], prim[3, x - 1]
        for k in range(5):
            jump = fast_u * (up[k] - s[k]) - fast_d * (s[k] - down[k])
            total.append(flux_of(up, vu, pu, 0, k) - flux_of(down, vd, pd, 0, k) - jump)
        for d, axis in ((1, 0), (2, 1)):
            size = s[0].shape[axis]
            v = prim[d, x]
            speed = jnp.abs(v) + sound
            fast = jnp.maximum(speed, pltpu.roll(speed, size - 1, axis))
            for k in range(5):
                flux = flux_of(s, v, p, d, k)
                face = flux + pltpu.roll(flux, size - 1, axis)
                face = face - fast * (pltpu.roll(s[k], size - 1, axis) - s[k])
                total[k] = total[k] + (face - pltpu.roll(face, 1, axis))
        for k in range(5):
            value = b_weight * s[k] - (0.5 * DT_FLOW * b_weight) * total[k]
            if a_weight is not None:
                value = value + a_weight * base[k, x]
            if rows is not None:
                value = value[:rows]
            dst[k, x - shift] = value
        return carry

    lax.fori_loop(first, last, advance, 0)


STAGES = ((None, 1.0), (0.75, 0.25), (1.0 / 3.0, 2.0 / 3.0))


def place(s0, start, mine, other, first=0):
    rows = mine.shape[2]
    for i in range(mine.shape[1]):
        for k in range(5):
            s0[k, start + first + i, :rows] = mine[k, i]
            s0[k, start + first + i, rows:] = other[k, i]


def around_own(planes):
    above = jnp.where(flags()[0] == 0, 2 * planes, 0)
    return above, 2 * planes - above


def first_flow_body(*refs):
    mine, other = refs[:3], refs[3:6]
    new_own, new_part, mid, low, high = refs[6:11]
    own_ref, part_ref, lo_ref, hi_ref = refs[11:15]
    s0, s1, s2, prim = refs[15:]
    planes, rows = mine[0].shape[1], mine[0].shape[2]
    for start, a, b in zip((planes, *around_own(planes)), mine, other):
        place(s0, start, a, b)
    wide = 3 * planes
    flow_stage(s0, None, s1, prim, 1, wide - 1, STAGES[0])
    flow_stage(s1, s0, s2, prim, 2, wide - 2, STAGES[1])
    flow_stage(s2, s0, s1, prim, 3, wide - 3, STAGES[2])
    for i in range(-1, planes + 1):
        x = planes + i
        inverse = 1.0 / s1[0, x]
        v = [s1[1 + d, x] * inverse for d in range(3)]
        for d in range(3):
            if i == -1:
                lo_ref[d, 0] = v[d][:rows]
            elif i == planes:
                hi_ref[d, 0] = v[d][:rows]
            else:
                own_ref[d, i] = v[d][:rows]
                part_ref[d, i] = v[d][rows:]
        for k in range(5):
            if i == -1:
                low[k, 0] = s1[k, x]
            elif i == planes:
                high[k, 0] = s1[k, x]
            else:
                new_own[k, i] = s1[k, x, :rows]
                new_part[k, i] = s1[k, x, rows:]
                if 0 < i < planes - 1:
                    mid[k, i - 1] = s1[k, x, :rows]


def last_flow_body(*refs):
    own, part, low, high = refs[:4]
    even, odd, even_part, odd_part, out_ref = refs[4:9]
    s0, s1, s2, prim = refs[9:]
    planes, rows = own.shape[1], own.shape[2]
    place(s0, planes, own, part)
    even_at, odd_at = around_own(planes)
    place(s0, even_at, even, even_part, first=1)
    place(s0, odd_at, odd, odd_part, first=1)
    wide = 3 * planes
    for k in range(5):
        s0[k, planes - 1] = low[k, 0]
        s0[k, 2 * planes] = high[k, 0]
    flow_stage(s0, None, s1, prim, 2, wide - 2, STAGES[0])
    flow_stage(s1, s0, s2, prim, 3, wide - 3, STAGES[1])
    flow_stage(s2, s0, out_ref, prim, planes, 2 * planes, STAGES[2], shift=planes, rows=rows)


def derive(values):
    half = NP // 2
    even = [values[i] + values[NP - 1 - i] for i in range(half)]
    odd = [values[i] - values[NP - 1 - i] for i in range(half)]
    tops, bottoms = [], []
    for a in range(half):
        plus = minus = None
        for i in range(half):
            ce = 0.5 * float(MATRIX[a, i] + MATRIX[a, NP - 1 - i])
            co = 0.5 * float(MATRIX[a, i] - MATRIX[a, NP - 1 - i])
            te, to = ce * even[i], co * odd[i]
            plus = te if plus is None else plus + te
            minus = to if minus is None else minus + to
        tops.append(plus + minus)
        bottoms.append(minus - plus)
    return tops + bottoms[::-1]


def along_middle(ps, us, lanes):
    p = derive(ps)
    below, above = (ps[-1], -ps[0]) if us is None else (ps[-1] + us[-1], us[0] - ps[0])
    own_low, own_high = (ps[0], -ps[-1]) if us is None else (ps[0] + us[0], us[-1] - ps[-1])
    low = LIFT * (pltpu.roll(below, EZ, 1) - own_low)
    high = LIFT * (pltpu.roll(above, lanes - EZ, 1) - own_high)
    dp = [None] * NP if us is None else [-u for u in derive(us)]
    du = [-value for value in p]
    dp[0] = low if dp[0] is None else dp[0] + low
    dp[-1] = -high if dp[-1] is None else dp[-1] - high
    du[0] = du[0] + low
    du[-1] = du[-1] + high
    return dp, du


def inner_maker(coef, lanes):
    lane = lax.broadcasted_iota(jnp.int32, (NP, lanes), 1)
    row = lax.broadcasted_iota(jnp.int32, (NP, lanes), 0)
    firsts = (lane & (EZ - 1)) == 0
    lasts = (lane & (EZ - 1)) == EZ - 1
    is_low = row == 0
    lift_u = jnp.where(is_low | (row == NP - 1), LIFT, 0.0)
    lift_p = jnp.where(is_low, LIFT, jnp.where(row == NP - 1, -LIFT, 0.0))

    def slope(value):
        total = coef[0] * value
        for k in range(1, NP):
            total = total + coef[k] * pltpu.roll(value, NP - k, 0)
        return total

    def jump_of(p, u):
        up, down = (p, -p) if u is None else (u + p, u - p)
        edge = jnp.where(is_low, pltpu.roll(up, 1, 0), pltpu.roll(down, NP - 1, 0))
        from_low = jnp.where(firsts, pltpu.roll(edge, lanes + 1 - EZ, 1), pltpu.roll(edge, 1, 1))
        from_high = jnp.where(
            lasts, pltpu.roll(edge, EZ - 1, 1), pltpu.roll(edge, lanes - 1, 1)
        )
        return jnp.where(is_low, from_low - up, from_high - down)

    def both(p, u, want_u=True):
        jump = jump_of(p, u)
        dp = lift_p * jump if u is None else lift_p * jump - slope(u)
        return dp, (lift_u * jump - slope(p)) if want_u else None

    return both


def local_rate(s, r, coef, forcing=None):
    lanes = s.shape[-1]

    def first(j, carry):
        p = derive([s[0, i, j] for i in range(NP)])
        u = derive([s[1, i, j] for i in range(NP)])
        for i in range(NP):
            r[0, i, j] = -u[i]
            r[1, i, j] = -p[i] if forcing is None else forcing[0, i, j] - p[i]
        return carry

    lax.fori_loop(0, NP, first, 0)
    inner = inner_maker(coef, lanes)

    def second(i, carry):
        ps = [s[0, i, j] for j in range(NP)]
        dp, du = along_middle(ps, [s[2, i, j] for j in range(NP)], lanes)
        for j in range(NP):
            dq, dw = inner(ps[j], s[3, i, j])
            r[0, i, j] = r[0, i, j] + (dp[j] + dq)
            r[2, i, j] = du[j] if forcing is None else forcing[1, i, j] + du[j]
            r[3, i, j] = dw if forcing is None else forcing[2, i, j] + dw
        return carry

    lax.fori_loop(0, NP, second, 0)


def each(function):
    def body(i, carry):
        function(i)
        return carry

    lax.fori_loop(0, NP, body, 0)


LAST = NP - 1


def chosen(low, when_low, when_high):
    return jnp.where(low, when_low, when_high)


def add_lifts(s, r, incoming=None):
    def lift(j):
        from_low, from_high = (0.0, 0.0) if incoming is None else incoming(j)
        low = LIFT * (from_low - (s[1, 0, j] + s[0, 0, j]))
        high = LIFT * (from_high - (s[1, LAST, j] - s[0, LAST, j]))
        r[0, 0, j] = r[0, 0, j] + low
        r[1, 0, j] = r[1, 0, j] + low
        r[0, LAST, j] = r[0, LAST, j] - high
        r[1, LAST, j] = r[1, LAST, j] + high

    each(lift)


def ends_body(w, even, odd):
    low_core = flags()[1] == 0
    up, down = w[0, LAST] + w[1, LAST], w[1, 0] - w[0, 0]
    even[...] = chosen(low_core, up, down)
    odd[...] = chosen(low_core, down, up)


def rate_body(w, even, odd, coef, r):
    low_core = flags()[1] == 0
    local_rate(w, r, coef)
    add_lifts(
        w,
        r,
        lambda j: (
            chosen(low_core, odd[j], even[j]),
            chosen(low_core, even[j], odd[j]),
        ),
    )


def unpack_body(w, r0, arrived_hbm, coef, f_out, s1, even, odd, arrived, wide, sums, sems, f):
    lanes = w.shape[-1]
    groups = sums.shape[0]
    stride = groups * CAP + 1
    half = arrived.shape[0] // stride // 2
    loads = []
    for h in range(2):
        part = pl.ds(h * half * stride, half * stride)
        loads.append(pltpu.make_async_copy(arrived_hbm.at[part], arrived.at[part], sems.at[h]))
        loads[-1].start()
    row = lax.broadcasted_iota(jnp.int32, (lanes, half), 0).astype(F32)
    for h in range(2):
        loads[h].wait()
        base = h * half * stride
        labels = arrived[pl.ds(base + stride - 1, half, stride=stride), :].T
        pick = jnp.concatenate(
            [(row == labels[s : s + 1] - 1.0).astype(F32).astype(BF16) for s in range(CAP)],
            axis=1,
        )
        for g in range(groups):
            for s in range(CAP):
                part = arrived[pl.ds(base + CAP * g + s, half, stride=stride), :]
                high, low = halves(part)
                wide[g % 2, s * half : (s + 1) * half, 0:128] = high
                wide[g % 2, s * half : (s + 1) * half, 128:256] = low
            both = dot(pick, wide[g % 2])
            if h == 0:
                sums[g] = both
                continue
            both = both + sums[g]
            nodes = (both[:, :128] + both[:, 128:]).T
            for row_of in range(128 // NP):
                at = g * 128 // NP + row_of
                c, i, j = at // (NP * NP), at // NP % NP, at % NP
                f[c, i, j] = nodes[row_of * NP : (row_of + 1) * NP, :]
    keep = pltpu.make_async_copy(f, f_out, sems.at[2])
    keep.start()

    def add(i):
        for k in range(4):
            rate = r0[k, i] if k == 0 else r0[k, i] + f[k - 1, i]
            s1[k, i] = w[k, i] + DT_WAVE * rate

    each(add)
    inner = inner_maker(coef, lanes)
    low_core = flags()[1] == 0
    now, then = [], []
    for i, sign in ((LAST, 1.0), (0, -1.0)):
        ps = [s1[0, i, j] for j in range(NP)]
        dp, _ = along_middle(ps, [s1[2, i, j] for j in range(NP)], lanes)
        now_rows, then_rows = [], []
        for j in range(NP):
            dq, _ = inner(ps[j], s1[3, i, j], want_u=False)
            rate_p = dp[j] + dq
            rate_u = f[0, i, j]
            for m in range(NP):
                c = float(MATRIX[i, m])
                if c != 0.0:
                    rate_p = rate_p - c * s1[1, m, j]
                    rate_u = rate_u - c * s1[0, m, j]
            u = s1[1, i, j]
            next_p = 0.75 * w[0, i, j] + 0.25 * (ps[j] + DT_WAVE * rate_p)
            next_u = 0.75 * w[1, i, j] + 0.25 * (u + DT_WAVE * rate_u)
            now_rows.append(u + sign * ps[j])
            then_rows.append(next_u + sign * next_p)
        now.append(now_rows)
        then.append(then_rows)
    for j in range(NP):
        for slot, (up, down) in enumerate((now, then)):
            even[slot, j] = chosen(low_core, up[j], down[j])
            odd[slot, j] = chosen(low_core, down[j], up[j])
    keep.wait()


def middle_body(w, s1, f, coef, s2, r2, r1):
    local_rate(s1, r1, coef, f)
    add_lifts(s1, r1)

    def add(i):
        for k in range(4):
            s2[k, i] = 0.75 * w[k, i] + 0.25 * (s1[k, i] + DT_WAVE * r1[k, i])

    each(add)
    local_rate(s2, r2, coef, f)
    add_lifts(s2, r2)


def relay_body(w, s1, f, coef, even, odd, s2, r2, even3, odd3, far_even, far_odd, r1):
    middle_body(w, s1, f, coef, s2, r2, r1)
    low_flow, low_core = flags()[0] == 0, flags()[1] == 0

    def third(k, i, j):
        return w[k, i, j] * (1.0 / 3.0) + (2.0 / 3.0) * (s2[k, i, j] + DT_WAVE * r2[k, i, j])

    def send(j):
        for slot in range(2):
            even3[slot, j] = even[slot, j]
            odd3[slot, j] = odd[slot, j]
        up = third(1, LAST, j) + third(0, LAST, j)
        down = third(1, 0, j) - third(0, 0, j)
        even3[2, j] = chosen(low_core, up, down)
        odd3[2, j] = chosen(low_core, down, up)
        up = chosen(low_core, even[0, j], odd[0, j])
        down = chosen(low_core, odd[0, j], even[0, j])
        far_even[j] = chosen(low_flow, up, down)
        far_odd[j] = chosen(low_flow, down, up)

    each(send)


def close_step(w, s2, r2, even, odd, coef, out, s, r):
    lanes = w.shape[-1]
    low_core = flags()[1] == 0

    def first(j):
        low = (0.25 * DT_WAVE * LIFT) * chosen(low_core, odd[0, j], even[0, j])
        high = (0.25 * DT_WAVE * LIFT) * chosen(low_core, even[0, j], odd[0, j])
        s[0, j] = low
        s[1, j] = -high
        lift_low = LIFT * (chosen(low_core, odd[1, j], even[1, j]) - 2.0 * low)
        lift_high = LIFT * (chosen(low_core, even[1, j], odd[1, j]) - 2.0 * high)
        for i in range(NP):
            a, b = float(MATRIX[i, 0]), float(MATRIX[i, LAST])
            p = r2[0, i, j] - a * low - b * high
            u = r2[1, i, j] - a * low + b * high
            if i == 0:
                p, u = p + lift_low, u + lift_low
            if i == LAST:
                p, u = p - lift_high, u + lift_high
            r[0, i, j] = p
            r[1, i, j] = u

    each(first)
    third = 1.0 / 3.0

    def close(k, i, j, state, rate):
        out[k, i, j] = w[k, i, j] * third + (2.0 * third) * (state + DT_WAVE * rate)

    def inside(i, carry):
        for j in range(NP):
            for k in range(4):
                rate = r[k, i, j] if k < 2 else r2[k, i, j]
                close(k, i, j, s2[k, i, j], rate)
        return carry

    lax.fori_loop(1, LAST, inside, 0)
    inner = inner_maker(coef, lanes)
    for side, i in ((0, 0), (1, LAST)):
        ps = [s[side, j] for j in range(NP)]
        dp, du = along_middle(ps, None, lanes)
        for j in range(NP):
            dq, dw = inner(ps[j], None)
            rate = r[0, i, j] + dq
            if dp[j] is not None:
                rate = rate + dp[j]
            close(0, i, j, s2[0, i, j] + ps[j], rate)
            change = ps[j] if side == 0 else -ps[j]
            close(1, i, j, s2[1, i, j] + change, r[1, i, j])
            close(2, i, j, s2[2, i, j], r2[2, i, j] + du[j])
            close(3, i, j, s2[3, i, j], r2[3, i, j] + dw)


def turn_body(
    w, s2, r2, even, odd, far_even, far_odd, own_even, own_odd, coef, out, r0, s, r, q
):
    close_step(w, s2, r2, even, odd, coef, out, s, r)
    lanes = w.shape[-1]
    low_flow, low_core = flags()[0] == 0, flags()[1] == 0
    inner = inner_maker(coef, lanes)
    weight = 0.25 * DT_WAVE * LIFT

    def spill(values):
        dp, _ = along_middle(values, None, lanes)
        found = []
        for j in range(NP):
            dq, _ = inner(values[j], None, want_u=False)
            found.append(dq if dp[j] is None else dp[j] + dq)
        return found

    ups = [weight * chosen(low_core, own_even[0, j], own_odd[0, j]) for j in range(NP)]
    downs = [weight * chosen(low_core, own_odd[0, j], own_even[0, j]) for j in range(NP)]
    step = 2.0 / 3.0 * DT_WAVE
    for j, (a, b) in enumerate(zip(spill([-d for d in downs]), spill(ups))):
        far_low = chosen(low_flow, far_odd[j], far_even[j])
        far_high = chosen(low_flow, far_even[j], far_odd[j])
        a = a - (2.0 * float(MATRIX[LAST, 0]) * weight) * far_low
        b = (2.0 * float(MATRIX[0, LAST]) * weight) * far_high - b
        q[0, j] = chosen(low_core, odd[2, j], even[2, j]) + step * a
        q[1, j] = chosen(low_core, even[2, j], odd[2, j]) + step * b
    local_rate(out, r0, coef)
    add_lifts(out, r0, lambda j: (q[0, j], q[1, j]))


def trade(value, axis, odd):
    size = lax.axis_size(axis)
    pairs = []
    for i in range(odd, size + odd, 2):
        a, b = i % size, (i + 1) % size
        pairs += [(a, b), (b, a)]
    return lax.ppermute(value, axis, pairs)


def exchange_all(value):
    return lax.all_to_all(value, AXES, split_axis=0, concat_axis=0, tiled=True)


def advance(density, velocity, pressure, wave, tables, margin_element, margin_block, margin_table):
    planes, rows, width = density.shape
    lanes = wave.shape[-1]
    devices = lax.axis_size("flow") * lax.axis_size("group")
    kinds, nodes = tables.shape[:2]

    coef = np.stack([MATRIX[np.arange(NP), (np.arange(NP) + k) % NP] for k in range(NP)])
    coef = jnp.asarray(np.broadcast_to(coef[:, :, None], (NP, NP, lanes)).copy())
    odd_flow = lax.axis_index("flow") & 1

    inward = (planes - 1) * (1 - odd_flow)
    v_even = trade(lax.dynamic_slice_in_dim(velocity, inward, 1, 1), "flow", 0)
    v_odd = trade(lax.dynamic_slice_in_dim(velocity, planes - 1 - inward, 1, 1), "flow", 1)
    v_part = trade(velocity, "group", 0)

    block = sds(5, planes, rows, width)
    fields, margin = call(
        fields_body,
        (block, sds(8, margin_element.shape[1], dtype=jnp.int32)),
        1_000_000,
        limit=WHOLE_VMEM,
    )(density, velocity, pressure, margin_element, margin_block, margin_table)

    def surround(own):
        even = trade(own, "flow", 0)
        return (own, even, trade(own, "flow", 1))

    def swap_rows(pieces):
        return [trade(p, "group", 0) for p in pieces]

    pieces = surround(fields)
    others = swap_rows(pieces)

    def send(speeds, extra, length, out_shape=(), **keys):
        sent = sds(devices * length, 128)
        sent = call(
            lambda *refs: pack_body(*refs, paired=bool(out_shape)),
            (sent, *out_shape) if out_shape else sent,
            8_000_000,
            scratch=(
                *(pltpu.VMEM(o.shape, o.dtype) for o in out_shape),
                pltpu.VMEM((2, 3 * planes * rows, 128), F32),
                pltpu.VMEM((3, 256, nodes), BF16),
                pltpu.VMEM(tables.shape, F32),
                pltpu.VMEM((devices * length, 128), F32),
                pltpu.SemaphoreType.DMA((kinds + 4,)),
            ),
            limit=PACK_VMEM,
            **keys,
        )(*speeds, tables, *extra)
        sent, *kept = sent if out_shape else (sent,)
        sent = exchange_all(sent.reshape(devices, 1, length * 128))
        return sent.reshape(devices * length, 128), kept

    stride = 3 * CAP * nodes // 128 + 1
    arrived_1, kept = send(
        (velocity, v_part, v_even, v_odd),
        (margin,),
        stride,
        (sds(CAP * devices, 256, dtype=BF16), sds(devices, 128)),
        specs="vvvvhv",
        out_specs="hhh",
    )

    speed = sds(3, planes, rows, width)
    thin = sds(3, 1, rows, width)
    edge = sds(5, 1, 2 * rows, width)
    wide = pltpu.VMEM((5, 3 * planes, 2 * rows, width), F32)
    new_own, new_part, mid, low_edge, high_edge, own, part, low, high = call(
        first_flow_body,
        (block, block, sds(5, planes - 2, rows, width), edge, edge, speed, speed, thin, thin),
        60_000_000,
        scratch=[wide] * 4,
    )(*pieces, *others)
    arrived_2, _ = send((own, part, high, low), kept, stride, specs="vvvvhvv", out_specs="h")
    mids = surround(mid)[1:]

    def finish_flow(mids):
        return call(last_flow_body, block, 30_000_000, scratch=[wide] * 4)(
            new_own, new_part, low_edge, high_edge, *mids, *swap_rows(mids)
        )

    state = sds(*wave.shape)
    force = sds(3, *wave.shape[1:])
    hold = pltpu.VMEM(wave.shape, F32)
    face = sds(NP, NP, lanes)
    pair = sds(2, NP, NP, lanes)
    triple = sds(3, NP, NP, lanes)
    sides = pltpu.VMEM((2, NP, NP, lanes), F32)
    couple = pltpu.VMEM((2,) + wave.shape[1:], F32)
    unpack = call(
        unpack_body,
        (force, state, pair, pair),
        12_000_000,
        scratch=[
            pltpu.VMEM((devices * stride, 128), F32),
            pltpu.VMEM((2, CAP * devices // 2, 256), BF16),
            pltpu.VMEM((3 * nodes // 128, lanes, 256), F32),
            pltpu.SemaphoreType.DMA((3,)),
            pltpu.VMEM((3, *wave.shape[1:]), F32),
        ],
        specs="vvhv",
        out_specs="hvvv",
    )

    def around(even, odd):
        return (trade(even, "group", 0), trade(odd, AXES, 1))

    ends = call(ends_body, (face, face), 100_000)(wave)
    faces = around(*ends)
    rate = call(rate_body, state, 8_000_000)(wave, *faces, coef)
    forcing, s1, *ends = unpack(wave, rate, arrived_1, coef)
    s2, r2, even, odd, far_even, far_odd = call(
        relay_body, (state, state, triple, triple, face, face), 16_000_000, scratch=[hold]
    )(wave, s1, forcing, coef, *ends)
    faces = around(even, odd)
    far = (trade(far_even, "flow", 0), trade(far_odd, "flow", 1))
    mids, _ = lax.optimization_barrier((mids, far_even))
    flow_state = finish_flow(mids)
    wave, rate = call(
        turn_body, (state, state), 14_000_000, scratch=[sides, couple, sides]
    )(wave, s2, r2, *faces, *far, *ends, coef)

    forcing, s1, *ends = unpack(wave, rate, arrived_2, coef)
    faces = around(*ends)
    s2, r2 = call(middle_body, (state, state), 16_000_000, scratch=[hold])(wave, s1, forcing, coef)
    wave = call(close_step, state, 6_000_000, scratch=[sides, couple])(wave, s2, r2, *faces, coef)
    return (flow_state, wave, forcing)


def solution(mesh):
    in_specs = (
        P("flow", "group", None),
        P(None, "flow", "group", None),
        P("flow", "group", None),
        P(None, None, None, None, AXES),
        P(),
        P(AXES, None),
        P(AXES, None),
        P(AXES, None),
    )
    out_specs = (
        P(None, "flow", "group", None),
        P(None, None, None, None, AXES),
        P(None, None, None, None, AXES),
    )
    return jax.shard_map(advance, mesh=mesh, in_specs=in_specs, out_specs=out_specs, check_vma=False)
```
